32 devices in a mesh: rows: 8 (over z, core), seq: 4 (over y, x).
Axes of the slice: x: 2, y: 2, z: 4, core: 2. Of those that a mesh axis runs over, the one named last changes fastest.
Arguments:
- tokens: bfloat16 [16, 2048, 1152], P('rows', 'seq'), may hold values from -6 to 6
- picture_ids: int32 [16, 2048], P('rows'), may hold values from -1 to 19, as said below
- attn_gain: bfloat16 [1152], P('rows'), may hold values from 0.099609375 to 1.8984375
- attn_shift: bfloat16 [1152], P('rows'), may hold values from -3 to 3
- query_weight: bfloat16 [1152, 1152], P('rows'), may hold values from -0.1875 to 0.1875
- query_bias: bfloat16 [1152], P('rows'), may hold values from -3 to 3
- key_weight: bfloat16 [1152, 1152], P('rows'), may hold values from -0.1875 to 0.1875
- value_weight: bfloat16 [1152, 1152], P('rows'), may hold values from -0.1875 to 0.1875
- value_bias: bfloat16 [1152], P('rows'), may hold values from -3 to 3
- output_weight: bfloat16 [1152, 1152], P('rows'), may hold values from -2 to 2
- output_bias: bfloat16 [1152], P('rows'), may hold values from -3 to 3
- mlp_gain: bfloat16 [1152], P('rows'), may hold values from 0.099609375 to 1.8984375
- mlp_shift: bfloat16 [1152], P('rows'), may hold values from -3 to 3
- up_weight: bfloat16 [1152, 4304], P('rows'), may hold values from -0.1875 to 0.1875
- up_bias: bfloat16 [4304], P('rows'), may hold values from -3 to 3
- down_weight: bfloat16 [4304, 1152], P(None, 'rows'), may hold values from -0.09375 to 0.09375
- down_bias: bfloat16 [1152], P('rows'), may hold values from -3 to 3
- cotangent: bfloat16 [16, 2048, 1152], P('rows', 'seq'), may hold values from -6 to 6
Outputs:
- activations: float32 [16, 2048, 1152], P('rows', 'seq')
- token_grad: float32 [16, 2048, 1152], P('rows', 'seq')
- grad_attn_gain: float32 [1152], P('rows')
- grad_attn_shift: float32 [1152], P('rows')
- grad_query_weight: float32 [1152, 1152], P('rows')
- grad_query_bias: float32 [1152], P('rows')
- grad_key_weight: float32 [1152, 1152], P('rows')
- grad_value_weight: float32 [1152, 1152], P('rows')
- grad_value_bias: float32 [1152], P('rows')
- grad_output_weight: float32 [1152, 1152], P('rows')
- grad_output_bias: float32 [1152], P('rows')
- grad_mlp_gain: float32 [1152], P('rows')
- grad_mlp_shift: float32 [1152], P('rows')
- grad_up_weight: float32 [1152, 4304], P('rows')
- grad_up_bias: float32 [4304], P('rows')
- grad_down_weight: float32 [4304, 1152], P(None, 'rows')
- grad_down_bias: float32 [1152], P('rows')
The draws below stay inside these ranges and needn't reach their ends.
Inputs may be any that keep to these rules, and one draw needn't show every extreme that they name: `picture_ids`: each row of 2048 slots holds whole pictures of 100 to 1024 patches, numbered 0, 1, 2, ... from the row's start, then pad slots numbered -1 to the row's end. The first row begins with a picture of exactly 1024 patches; the last row holds 20 pictures of exactly 100 patches, then pads.
All inputs are finite; a program needn't handle non-finite values.
Results may differ from the reference program's by a relative error of at most 0.019.
Values may be sent and summed in bfloat16 or wider, within the bound.
A program may use at most 256 MiB of HBM per device.

```python
import jax
import jax.numpy as jnp
from jax import lax

MODEL_WIDTH = 1152
ATTENTION_HEADS = 16
HEAD_SIZE = 72
FF = 4304
ROW_SLOTS = 2048
FEWEST_PATCHES = 100
MAXPIC = 1024
PACKED_ROWS = 16


def draw_picture_ids(key, part):
    most_pictures = ROW_SLOTS // FEWEST_PATCHES + 1
    lengths = jax.random.randint(key, (PACKED_ROWS, most_pictures), FEWEST_PATCHES, MAXPIC + 1)
    lengths = lengths.at[PACKED_ROWS - 1].set(FEWEST_PATCHES)
    lengths = lengths.at[0, 0].set(MAXPIC)
    picture_ends = jnp.cumsum(lengths, axis=1)
    kept_entries = picture_ends <= ROW_SLOTS
    filled = jnp.sum(jnp.where(kept_entries, lengths, 0), axis=1)
    slot_places = jnp.arange(ROW_SLOTS, dtype=jnp.int32)
    before = (picture_ends[:, None, :] <= slot_places[None, :, None]) & kept_entries[:, None, :]
    counted = jnp.sum(before.astype(jnp.int32), axis=2)
    return jnp.where(slot_places[None, :] < filled[:, None], counted, -1).astype(jnp.int32)


def block_scale(stream_key, dims, shards, low, high):
    factor_of, own = 1.0, jax.random.fold_in(stream_key, 6)
    for position, parts in shards:
        heights = jnp.exp(jax.random.uniform(jax.random.fold_in(own, position), (parts,), jnp.float32, low / len(shards), high / len(shards)))
        factor_of = factor_of * jnp.repeat(heights, dims[position] // parts).reshape([-1 if axis == position else 1 for axis in range(len(dims))])
    return factor_of


def bell_draw(stream_key, dims, scale, most, pieces=(), kind=jnp.bfloat16):
    values = jax.random.normal(stream_key, dims, jnp.float32) * scale
    if len(pieces) > 0:
        values = block_scale(stream_key, dims, pieces, -0.22, 0.18) * values
    return jnp.clip(values, min=-most, max=most).astype(kind)


def setup_inputs(seed: int = 0) -> dict:
    keys = jax.random.split(jax.random.key(seed), 19)
    tokens = bell_draw(keys[0], (PACKED_ROWS, ROW_SLOTS, MODEL_WIDTH), 1.0, 6.0, ((0, 8), (1, 4)))
    picture_ids = draw_picture_ids(jax.random.fold_in(keys[18], 71), 0)
    attn_gain = jnp.clip(1.0 + 0.18 * jax.random.normal(keys[2], (MODEL_WIDTH,), jnp.float32), 0.099609375, 1.8984375).astype(jnp.bfloat16)
    attn_shift = bell_draw(keys[3], (MODEL_WIDTH,), 0.5, 3.0, ((0, 8),))
    query_weight = bell_draw(keys[4], (MODEL_WIDTH, MODEL_WIDTH), MODEL_WIDTH ** -0.5, 0.1875, ((0, 8),))
    query_bias = bell_draw(keys[5], (MODEL_WIDTH,), 0.5, 3.0, ((0, 8),))
    key_weight = bell_draw(keys[6], (MODEL_WIDTH, MODEL_WIDTH), MODEL_WIDTH ** -0.5, 0.1875, ((0, 8),))
    value_weight = bell_draw(keys[7], (MODEL_WIDTH, MODEL_WIDTH), MODEL_WIDTH ** -0.5, 0.1875, ((0, 8),))
    value_bias = bell_draw(keys[8], (MODEL_WIDTH,), 0.5, 3.0, ((0, 8),))
    output_weight = bell_draw(keys[9], (MODEL_WIDTH, MODEL_WIDTH), (max(MODEL_WIDTH // 128, 1)) ** -0.5, 2.0, ((0, 8),))
    output_bias = bell_draw(keys[10], (MODEL_WIDTH,), 0.5, 3.0, ((0, 8),))
    mlp_gain = jnp.clip(1.0 + 0.18 * jax.random.normal(keys[11], (MODEL_WIDTH,), jnp.float32), 0.099609375, 1.8984375).astype(jnp.bfloat16)
    mlp_shift = bell_draw(keys[12], (MODEL_WIDTH,), 0.5, 3.0, ((0, 8),))
    up_weight = bell_draw(keys[13], (MODEL_WIDTH, FF), MODEL_WIDTH ** -0.5, 0.1875, ((0, 8),))
    up_bias = bell_draw(keys[14], (FF,), 0.5, 3.0, ((0, 8),))
    down_weight = bell_draw(keys[15], (FF, MODEL_WIDTH), FF ** -0.5, 0.09375, ((1, 8),))
    down_bias = bell_draw(keys[16], (MODEL_WIDTH,), 0.5, 3.0, ((0, 8),))
    cotangent = bell_draw(keys[17], (PACKED_ROWS, ROW_SLOTS, MODEL_WIDTH), 1.0, 6.0, ((0, 8), (1, 4)))
    return {"tokens": tokens, "picture_ids": picture_ids, "attn_gain": attn_gain, "attn_shift": attn_shift, "query_weight": query_weight, "query_bias": query_bias, "key_weight": key_weight, "value_weight": value_weight, "value_bias": value_bias, "output_weight": output_weight, "output_bias": output_bias, "mlp_gain": mlp_gain, "mlp_shift": mlp_shift, "up_weight": up_weight, "up_bias": up_bias, "down_weight": down_weight, "down_bias": down_bias, "cotangent": cotangent}


@jax.custom_vjp
def lower_precision(v):
    return lax.optimization_barrier(v.astype(jnp.bfloat16)).astype(jnp.float32)

@jax.custom_vjp
def lower_backward(v):
    return v

def low_keep(v):
    return (lower_precision(v), None)

def low_pass(kept_entries, grad):
    return (grad,)

def back_keep(v):
    return (v, None)

def back_low(kept_entries, grad):
    return (lower_precision(grad),)
lower_precision.defvjp(low_keep, low_pass)
lower_backward.defvjp(back_keep, back_low)
EPS = 1e-06
HIGH = lax.Precision.HIGHEST

def layer_norm(value_rows, gain, shift):
    center = value_rows - lax.optimization_barrier(jnp.mean(value_rows, axis=-1, keepdims=True))
    spread = lax.optimization_barrier(jnp.mean(center * center, axis=-1, keepdims=True))
    return center * lax.rsqrt(spread + EPS) * gain + shift

def attend_block(query_block, id_block, key_rows, value_rows, picture_of_row):
    scores = jnp.einsum('qhd,khd->hqk', query_block, key_rows, precision=HIGH) * HEAD_SIZE ** (-0.5)
    scores = lower_backward(scores)
    allowed = (id_block[:, None] == picture_of_row[None, :])[None]
    scores = jnp.where(allowed, scores, -1e+30)
    highest = lax.optimization_barrier(jnp.max(scores, axis=-1, keepdims=True))
    expo = jnp.exp(scores - highest)
    probs = lower_precision(expo / lax.optimization_barrier(jnp.sum(expo, axis=-1, keepdims=True)))
    return jnp.einsum('hqk,khd->qhd', probs, value_rows, precision=HIGH)

def forward(params, token_row, picture_of_row):
    attn_gain, attn_shift, query_weight, query_bias, key_weight, value_weight, value_bias, output_weight, output_bias, mlp_gain, mlp_shift, up_weight, up_bias, down_weight, down_bias = params
    attn_input = lower_precision(layer_norm(token_row, attn_gain, attn_shift))
    query_rows = lower_precision(lower_backward(jnp.dot(attn_input, query_weight, precision=HIGH) + query_bias))
    key_rows = lower_precision(lower_backward(jnp.dot(attn_input, key_weight, precision=HIGH)))
    value_rows = lower_precision(lower_backward(jnp.dot(attn_input, value_weight, precision=HIGH) + value_bias))
    query_rows = query_rows.reshape(ROW_SLOTS, ATTENTION_HEADS, HEAD_SIZE)
    key_rows = key_rows.reshape(ROW_SLOTS, ATTENTION_HEADS, HEAD_SIZE)
    value_rows = value_rows.reshape(ROW_SLOTS, ATTENTION_HEADS, HEAD_SIZE)
    tile_block = min(512, ROW_SLOTS)
    query_tiles = query_rows.reshape(ROW_SLOTS // tile_block, tile_block, ATTENTION_HEADS, HEAD_SIZE)
    picture_id_blocks = picture_of_row.reshape(ROW_SLOTS // tile_block, tile_block)
    mixed_heads = lax.map(lambda member: jax.checkpoint(attend_block)(member[0], member[1], key_rows, value_rows, picture_of_row), (query_tiles, picture_id_blocks))
    mixed_heads = lower_precision(lower_backward(mixed_heads.reshape(ROW_SLOTS, MODEL_WIDTH)))
    attn_out = lower_backward(jnp.dot(mixed_heads, output_weight, precision=HIGH) + output_bias)
    resid = token_row + attn_out
    mlp_input = lower_precision(layer_norm(resid, mlp_gain, mlp_shift))
    hidden = lower_backward(jnp.dot(mlp_input, up_weight, precision=HIGH) + up_bias)
    gelu_out = lower_precision(jax.nn.gelu(hidden, approximate=True))
    return resid + jnp.dot(gelu_out, down_weight, precision=HIGH) + down_bias

def reference(tokens, picture_ids, attn_gain, attn_shift, query_weight, query_bias, key_weight, value_weight, value_bias, output_weight, output_bias, mlp_gain, mlp_shift, up_weight, up_bias, down_weight, down_bias, cotangent):
    params = tuple((weight.astype(jnp.float32) for weight in (attn_gain, attn_shift, query_weight, query_bias, key_weight, value_weight, value_bias, output_weight, output_bias, mlp_gain, mlp_shift, up_weight, up_bias, down_weight, down_bias)))

    def per_row(totals, inputs):
        token_row, picture_of_row, cot_row = inputs
        result, pullback = jax.vjp(lambda weights, value_rows: forward(weights, value_rows, picture_of_row), params, token_row.astype(jnp.float32))
        weight_grads, row_grad = pullback(cot_row.astype(jnp.float32))
        return (jax.tree.map(jnp.add, totals, weight_grads), (result, row_grad))
    zeros = tuple((jnp.zeros_like(weight) for weight in params))
    totals, (outputs, grads) = lax.scan(per_row, zeros, (tokens, picture_ids, cotangent))
    return (outputs, grads, totals[0], totals[1], totals[2], totals[3], totals[4], totals[5], totals[6], totals[7], totals[8], totals[9], totals[10], totals[11], totals[12], totals[13], totals[14])
```

```python
import functools
import jax
import jax.numpy as jnp
from jax import lax
from jax.experimental import pallas as pl
from jax.experimental.pallas import tpu as pltpu
from jax.sharding import PartitionSpec as P

HEAD_SIZE = 72
EPS = 1e-06
NEGATIVE = -1e30
LOG2E = 1.4426950408889634
PAD = 128
ROWS = 80


def split_refs(source, count, block):
    wide = source.astype(jnp.float32)
    return [wide[HEAD_SIZE * h : HEAD_SIZE * (h + 1)] for h in range(count)]


def grow_rows(value, rows):
    return jnp.concatenate([value, jnp.zeros((rows - value.shape[0], value.shape[1]), value.dtype)], axis=0)


def same_picture(kid_ref, qid_ref, key_start, query_start, block):
    key_ids = kid_ref[pl.ds(key_start, block), :]
    key_ids = jnp.concatenate([key_ids] * (block // 128), axis=1)
    return key_ids == qid_ref[0:1, pl.ds(query_start, block)]


def attend_kernel(low_ref, high_ref, qkv_ref, kid_ref, qid_ref, out_ref, log_ref, q_t, k_n, v_t, kept, top, total, acc, *, count, block):
    step = pl.program_id(0)
    length = qkv_ref.shape[2]
    factor = HEAD_SIZE ** (-0.5) * LOG2E

    @pl.when(step == 0)
    def _():
        @pl.loop(0, length // block)
        def _(part):
            at = pl.ds(pl.multiple_of(part * block, block), block)
            for h, value in enumerate(split_refs(qkv_ref[0, :, at], count, block)):
                q_t[h, :, at] = grow_rows(value, PAD).astype(jnp.bfloat16)
            for h, value in enumerate(split_refs(qkv_ref[1, :, at], count, block)):
                k_n[h, at, :] = grow_rows(value, PAD).T.astype(jnp.bfloat16)
            for h, value in enumerate(split_refs(qkv_ref[2, :, at], count, block)):
                v_t[h, :, at] = grow_rows(value, ROWS).astype(jnp.bfloat16)

    top[...] = jnp.full(top.shape, NEGATIVE, jnp.float32)
    total[...] = jnp.zeros(total.shape, jnp.float32)
    acc[...] = jnp.zeros(acc.shape, jnp.float32)
    query_start = pl.multiple_of(step * block, block)
    queries = pl.ds(query_start, block)

    def first(index, _):
        key_start = pl.multiple_of(index * block, block)
        mask = same_picture(kid_ref, qid_ref, key_start, query_start, block)
        for h in range(count):
            scores = jnp.dot(
                k_n[h, pl.ds(key_start, block), :], q_t[h, :, queries], preferred_element_type=jnp.float32
            )
            scores = jnp.where(mask, scores * factor, NEGATIVE)
            kept[h, pl.ds(key_start, block), :] = scores
            top[h] = jnp.maximum(top[h], jnp.max(scores.reshape(block // 8, 8, block), axis=0))
        return 0

    lax.fori_loop(low_ref[step], high_ref[step], first, 0)
    highest = [jnp.max(top[h], axis=0, keepdims=True) for h in range(count)]

    def second(index, _):
        keys = pl.ds(pl.multiple_of(index * block, block), block)
        for h in range(count):
            probs = jnp.exp2(kept[h, keys, :] - highest[h])
            total[h] += jnp.sum(probs.reshape(block // 8, 8, block), axis=0)
            acc[h] += jnp.dot(v_t[h, :, keys], probs.astype(jnp.bfloat16), preferred_element_type=jnp.float32)
        return 0

    lax.fori_loop(low_ref[step], high_ref[step], second, 0)
    sums = [jnp.sum(total[h], axis=0, keepdims=True) for h in range(count)]
    for h in range(count):
        log_ref[h : h + 1, :] = highest[h] + jnp.log2(sums[h])
    out_ref[0] = jnp.concatenate([acc[h, :HEAD_SIZE] / sums[h] for h in range(count)], axis=0).astype(jnp.bfloat16)


def attend(qkv, low, high, key_ids, query_ids, chunk):
    _, width, length = qkv.shape
    count = width // HEAD_SIZE
    block = min(256, chunk)
    per = chunk // block
    whole = lambda *shape: pl.BlockSpec(shape, lambda i, *_: (0,) * len(shape))
    area = length * length * count // 2
    return pl.pallas_call(
        functools.partial(attend_kernel, count=count, block=block),
        name="attend",
        grid_spec=pltpu.PrefetchScalarGridSpec(
            num_scalar_prefetch=2,
            grid=(length // block,),
            in_specs=[whole(3, width, length), whole(length, 128), whole(8, length)],
            out_specs=[
                pl.BlockSpec((1, width, block), lambda i, *_: (i // per, 0, i % per)),
                pl.BlockSpec((max(8, count), block), lambda i, *_: (0, i)),
            ],
            scratch_shapes=[
                pltpu.VMEM((count, PAD, length), jnp.bfloat16),
                pltpu.VMEM((count, length, PAD), jnp.bfloat16),
                pltpu.VMEM((count, ROWS, length), jnp.bfloat16),
                pltpu.VMEM((count, length, block), jnp.float32),
                pltpu.VMEM((count, 8, block), jnp.float32),
                pltpu.VMEM((count, 8, block), jnp.float32),
                pltpu.VMEM((count, ROWS, block), jnp.float32),
            ],
        ),
        out_shape=[
            jax.ShapeDtypeStruct((length // chunk, width, chunk), jnp.bfloat16),
            jax.ShapeDtypeStruct((max(8, count), length), jnp.float32),
        ],
        compiler_params=pltpu.CompilerParams(vmem_limit_bytes=40 << 20),
        cost_estimate=pl.CostEstimate(flops=area * 800, transcendentals=area, bytes_accessed=8 * length * width),
    )(low, high, qkv, key_ids, query_ids)


def attend_back_kernel(
    low_ref, high_ref, qkv_ref, gm_ref, out_ref, log_ref, kid_ref, qid_ref, grad_ref,
    q_t, k_t, k_n, v_n, g_t, delta, gq, gk, gv, *, count, block,
):
    step = pl.program_id(0)
    length = qkv_ref.shape[2]
    chunk = gm_ref.shape[2]
    scale = HEAD_SIZE ** (-0.5)
    factor = scale * LOG2E

    @pl.when(step == 0)
    def _():
        gq[...] = jnp.zeros(gq.shape, jnp.float32)

        @pl.loop(0, length // block)
        def _(part):
            at = pl.ds(pl.multiple_of(part * block, block), block)
            for h, value in enumerate(split_refs(qkv_ref[0, :, at], count, block)):
                q_t[h, :, at] = grow_rows(value, PAD).astype(jnp.bfloat16)
            for h, value in enumerate(split_refs(qkv_ref[1, :, at], count, block)):
                value = grow_rows(value, PAD)
                k_t[h, :, at] = value[:ROWS].astype(jnp.bfloat16)
                k_n[h, at, :] = value.T.astype(jnp.bfloat16)
            for h, value in enumerate(split_refs(qkv_ref[2, :, at], count, block)):
                v_n[h, at, :] = grow_rows(value, PAD).T.astype(jnp.bfloat16)

        for piece in range(length // chunk):
            at = pl.ds(piece * chunk, chunk)
            grads = split_refs(gm_ref[piece], count, chunk)
            outs = split_refs(out_ref[piece], count, chunk)
            for h in range(count):
                g_t[h, :, at] = grow_rows(grads[h], PAD).astype(jnp.bfloat16)
                delta[h, :, at] = jnp.sum(grads[h] * outs[h], axis=0, keepdims=True)

    gk[...] = jnp.zeros(gk.shape, jnp.float32)
    gv[...] = jnp.zeros(gv.shape, jnp.float32)
    key_start = pl.multiple_of(step * block, block)
    keys = pl.ds(key_start, block)

    def one(index, _):
        query_start = pl.multiple_of(index * block, block)
        queries = pl.ds(query_start, block)
        mask = same_picture(kid_ref, qid_ref, key_start, query_start, block)
        for h in range(count):
            scores = jnp.dot(k_n[h, keys, :], q_t[h, :, queries], preferred_element_type=jnp.float32)
            probs = jnp.where(mask, jnp.exp2(scores * factor - log_ref[h : h + 1, queries]), 0.0)
            back = jnp.dot(v_n[h, keys, :], g_t[h, :, queries], preferred_element_type=jnp.float32)
            slope = (probs * (back - delta[h, :, queries])).astype(jnp.bfloat16)
            nt = (((1,), (1,)), ((), ()))
            gv[h] += lax.dot_general(
                g_t[h, :ROWS, queries], probs.astype(jnp.bfloat16), nt, preferred_element_type=jnp.float32
            )
            gk[h] += lax.dot_general(q_t[h, :ROWS, queries], slope, nt, preferred_element_type=jnp.float32)
            gq[h, :, queries] += jnp.dot(k_t[h, :, keys], slope, preferred_element_type=jnp.float32)
        return 0

    lax.fori_loop(low_ref[step], high_ref[step], one, 0)
    grad_ref[1, :, keys] = (jnp.concatenate([gk[h, :HEAD_SIZE] for h in range(count)], axis=0) * scale).astype(jnp.bfloat16)
    grad_ref[2, :, keys] = jnp.concatenate([gv[h, :HEAD_SIZE] for h in range(count)], axis=0).astype(jnp.bfloat16)

    @pl.when(step == pl.num_programs(0) - 1)
    def _():
        @pl.loop(0, length // block)
        def _(part):
            at = pl.ds(pl.multiple_of(part * block, block), block)
            grad_ref[0, :, at] = (
                jnp.concatenate([gq[h, :HEAD_SIZE, at] for h in range(count)], axis=0) * scale
            ).astype(jnp.bfloat16)


def attend_back(qkv, grad_mixed, mixed, logsum, low, high, key_ids, query_ids):
    _, width, length = qkv.shape
    chunk = mixed.shape[2]
    count = width // HEAD_SIZE
    block = min(256, chunk)
    whole = lambda *shape: pl.BlockSpec(shape, lambda i, *_: (0,) * len(shape))
    area = length * length * count // 2
    return pl.pallas_call(
        functools.partial(attend_back_kernel, count=count, block=block),
        name="attend_back",
        grid_spec=pltpu.PrefetchScalarGridSpec(
            num_scalar_prefetch=2,
            grid=(length // block,),
            in_specs=[
                whole(3, width, length),
                whole(*mixed.shape),
                whole(*mixed.shape),
                whole(max(8, count), length),
                whole(length, 128),
                whole(8, length),
            ],
            out_specs=whole(3, width, length),
            scratch_shapes=[
                pltpu.VMEM((count, PAD, length), jnp.bfloat16),
                pltpu.VMEM((count, ROWS, length), jnp.bfloat16),
                pltpu.VMEM((count, length, PAD), jnp.bfloat16),
                pltpu.VMEM((count, length, PAD), jnp.bfloat16),
                pltpu.VMEM((count, PAD, length), jnp.bfloat16),
                pltpu.VMEM((count, 1, length), jnp.float32),
                pltpu.VMEM((count, ROWS, length), jnp.float32),
                pltpu.VMEM((count, ROWS, block), jnp.float32),
                pltpu.VMEM((count, ROWS, block), jnp.float32),
            ],
        ),
        out_shape=jax.ShapeDtypeStruct((3, width, length), jnp.bfloat16),
        compiler_params=pltpu.CompilerParams(vmem_limit_bytes=60 << 20),
        cost_estimate=pl.CostEstimate(flops=area * 2000, transcendentals=area, bytes_accessed=16 * length * width),
    )(low, high, qkv, grad_mixed, mixed, logsum, key_ids, query_ids)


def block_ranges(ids, block):
    ids = jnp.where(ids < 0, 1 << 20, ids).reshape(-1, block)
    first, last = ids[:, 0], ids[:, -1]
    low = jnp.sum((last[None, :] < first[:, None]).astype(jnp.int32), axis=1)
    high = jnp.sum((first[None, :] <= last[:, None]).astype(jnp.int32), axis=1)
    return low, high


def norm_parts(value_rows):
    center = value_rows - jnp.mean(value_rows, axis=-1, keepdims=True)
    inverse = lax.rsqrt(jnp.mean(center * center, axis=-1, keepdims=True) + EPS)
    return center * inverse, inverse


def norm_back(grad, normed, inverse, gain):
    scaled = grad * gain
    flat = jnp.mean(scaled, axis=-1, keepdims=True)
    along = jnp.mean(scaled * normed, axis=-1, keepdims=True)
    return inverse * (scaled - flat - normed * along)


def contract(left, right, left_axis, right_axis):
    return lax.dot_general(left, right, (((left_axis,), (right_axis,)), ((), ())), preferred_element_type=jnp.float32)


def per_device(
    tokens, picture_ids, attn_gain, attn_shift, query_weight, query_bias, key_weight, value_weight, value_bias,
    output_weight, output_bias, mlp_gain, mlp_shift, up_weight, up_bias, down_weight, down_bias, cotangent,
    *, seq_count, row_count,
):
    count, chunk, width = tokens.shape
    length = chunk * seq_count
    part = width // seq_count
    place = lax.axis_index("seq")
    band = lax.axis_index("rows")
    block = min(256, chunk)
    f32, bf16 = jnp.float32, jnp.bfloat16

    def own_columns(weight):
        return lax.dynamic_slice_in_dim(weight, place * part, part, axis=1)

    heads_shard = jnp.concatenate([own_columns(query_weight), own_columns(key_weight), own_columns(value_weight)], axis=1)
    heads_weight = lax.all_gather(heads_shard, "rows", axis=0, tiled=True)
    small = [attn_gain, attn_shift, query_bias, value_bias, output_bias, mlp_gain, mlp_shift, down_bias, up_bias]
    sizes = [piece.shape[0] for piece in small]
    packed = jnp.concatenate(small)
    padded = -(-packed.shape[0] // 2048) * 2048
    packed = jnp.pad(packed, (0, padded - packed.shape[0])).reshape(padded // 128, 128)
    packed = lax.all_gather(packed, "rows", axis=0, tiled=False).reshape(row_count, padded).astype(f32)
    pieces, start = [], 0
    for size in sizes:
        pieces.append(packed[:, start : start + size].reshape(row_count * size))
        start += size
    gain1, shift1, query_off, value_off, output_off, gain2, shift2, down_off, up_off = pieces
    heads_off = jnp.concatenate(
        [
            lax.dynamic_slice_in_dim(query_off, place * part, part),
            jnp.zeros((part,), f32),
            lax.dynamic_slice_in_dim(value_off, place * part, part),
        ]
    )

    attn_inputs, packs, mixes, logs, tables, mixed_own = [], [], [], [], [], []
    for row in range(count):
        ids = picture_ids[row]
        low, high = block_ranges(ids, block)
        tables.append((low, high, jnp.broadcast_to(ids[:, None], (length, 128)), jnp.broadcast_to(ids[None], (8, length))))
        whole_row = lax.all_gather(tokens[row], "seq", axis=0, tiled=True)
        attn_input = (norm_parts(whole_row.astype(f32))[0] * gain1 + shift1).astype(bf16)
        pack = (contract(heads_weight, attn_input, 0, 1) + heads_off[:, None]).astype(bf16).reshape(3, part, length)
        mixed, logsum = attend(pack, *tables[row], chunk)
        attn_inputs.append(attn_input)
        packs.append(pack)
        mixes.append(mixed)
        logs.append(logsum)
        back = lax.all_to_all(mixed, "seq", split_axis=0, concat_axis=0, tiled=True)
        mixed_own.append(back.reshape(width, chunk))

    output_whole = lax.all_gather(output_weight, "rows", axis=0, tiled=True)
    up_whole = lax.all_gather(up_weight, "rows", axis=0, tiled=True)
    down_whole = lax.all_gather(down_weight.T, "rows", axis=0, tiled=True)

    resid = jnp.concatenate(
        [
            tokens[row].astype(f32) + (contract(mixed_own[row], output_whole, 0, 0) + output_off)
            for row in range(count)
        ],
        axis=0,
    )
    normed2, inverse2 = norm_parts(resid)
    mlp_input = (normed2 * gain2 + shift2).astype(bf16)
    hidden = contract(mlp_input, up_whole, 1, 0) + up_off
    gelu_out, pull = jax.vjp(lambda v: jax.nn.gelu(v, approximate=True), hidden)
    gelu_out = gelu_out.astype(bf16)
    slope = pull(jnp.ones_like(hidden))[0].astype(bf16)
    activations = resid + contract(gelu_out, down_whole, 1, 1) + down_off

    cot = cotangent.reshape(count * chunk, width)
    grad_down = contract(cot, gelu_out, 0, 0).astype(bf16)
    grad_hidden = (contract(cot, down_whole, 1, 0) * slope.astype(f32)).astype(bf16)
    grad_up = contract(mlp_input, grad_hidden, 0, 0).astype(bf16)
    grad_mlp_input = contract(grad_hidden, up_whole, 1, 1)
    down_share = lax.psum_scatter(grad_down, "rows", scatter_dimension=0, tiled=True)
    up_share = lax.psum_scatter(grad_up, "rows", scatter_dimension=0, tiled=True)
    grad_resid = cot.astype(f32) + norm_back(grad_mlp_input, normed2, inverse2, gain2)
    grad_attn = grad_resid.astype(bf16)

    grad_output = None
    for row in range(count):
        term = contract(mixed_own[row], grad_attn[row * chunk : (row + 1) * chunk], 1, 0)
        grad_output = term if grad_output is None else grad_output + term
    output_share = lax.psum_scatter(grad_output.astype(bf16), "rows", scatter_dimension=0, tiled=True)
    grad_heads, grad_query_off, grad_value_off, token_grads, normed1_all, grad_in_all = None, 0.0, 0.0, [], [], []
    for row in range(count):
        grad_mixed = contract(output_whole, grad_attn[row * chunk : (row + 1) * chunk], 1, 1).astype(bf16)
        grad_mixed = lax.all_to_all(
            grad_mixed.reshape(seq_count, part, chunk), "seq", split_axis=0, concat_axis=0, tiled=True
        )
        grad_pack = attend_back(packs[row], grad_mixed, mixes[row], logs[row], *tables[row])
        grad_query_off = grad_query_off + jnp.sum(grad_pack[0].astype(f32), axis=1)
        grad_value_off = grad_value_off + jnp.sum(grad_pack[2].astype(f32), axis=1)
        grad_pack = grad_pack.reshape(3 * part, length)
        grad_in = contract(grad_pack, heads_weight, 0, 1).astype(bf16).reshape(seq_count, chunk, width)
        grad_in = lax.all_to_all(grad_in, "seq", split_axis=0, concat_axis=0, tiled=True)
        grad_in_all.append(jnp.sum(grad_in.astype(f32), axis=0))
        term = contract(attn_inputs[row], grad_pack, 0, 1)
        grad_heads = term if grad_heads is None else grad_heads + term
    heads_share = lax.psum_scatter(grad_heads.astype(bf16), "rows", scatter_dimension=0, tiled=True)

    grad_attn_input = jnp.concatenate(grad_in_all, axis=0)
    normed1, inverse1 = norm_parts(tokens.reshape(count * chunk, width).astype(f32))
    token_grad = grad_resid + norm_back(grad_attn_input, normed1, inverse1, gain1)

    def placed(value):
        return lax.dynamic_update_slice_in_dim(jnp.zeros((width,), f32), value, place * part, axis=0)

    grads = [
        jnp.sum(grad_attn_input * normed1, axis=0),
        jnp.sum(grad_attn_input, axis=0),
        placed(grad_query_off),
        placed(grad_value_off),
        jnp.sum(grad_attn.astype(f32), axis=0),
        jnp.sum(grad_mlp_input * normed2, axis=0),
        jnp.sum(grad_mlp_input, axis=0),
        jnp.sum(cot.astype(f32), axis=0),
        jnp.sum(grad_hidden.astype(f32), axis=0),
    ]
    together = jnp.concatenate([value.reshape(row_count, -1) for value in grads], axis=1)
    together = lax.psum(together, ("rows", "seq"))
    mine = lax.dynamic_index_in_dim(together, band, axis=0, keepdims=False)
    vectors, start = [], 0
    for size in sizes:
        vectors.append(mine[start : start + size])
        start += size

    def seq_sum(share):
        return jnp.sum(lax.all_gather(share, "seq", axis=0, tiled=False).astype(f32), axis=0)

    heads_all = lax.all_gather(heads_share, "seq", axis=0, tiled=False).astype(f32)

    def take(which):
        piece = heads_all[:, :, which * part : (which + 1) * part]
        return piece.transpose(1, 0, 2).reshape(heads_share.shape[0], width)

    return (
        activations.reshape(count, chunk, width),
        token_grad.reshape(count, chunk, width),
        vectors[0],
        vectors[1],
        take(0),
        vectors[2],
        take(1),
        take(2),
        vectors[3],
        seq_sum(output_share),
        vectors[4],
        vectors[5],
        vectors[6],
        seq_sum(up_share),
        vectors[8],
        seq_sum(down_share).T,
        vectors[7],
    )


def solution(mesh):
    matrix, vector, batch = P("rows", None), P("rows"), P("rows", "seq", None)
    columns = P(None, "rows")
    return jax.shard_map(
        functools.partial(per_device, seq_count=mesh.shape["seq"], row_count=mesh.shape["rows"]),
        mesh=mesh,
        in_specs=(
            batch, matrix, vector, vector, matrix, vector, matrix, matrix, vector, matrix, vector, vector, vector, matrix,
            vector, columns, vector, batch,
        ),
        out_specs=(
            batch, batch, vector, vector, matrix, vector, matrix, matrix, vector, matrix, vector, vector, vector, matrix,
            vector, columns, vector,
        ),
        check_vma=False,
    )
```

```python
import functools
import jax
import jax.numpy as jnp
from jax import lax
from jax.experimental import pallas as pl
from jax.experimental.pallas import tpu as pltpu
from jax.sharding import PartitionSpec as P


HEAD_SIZE = 72
EPS = 1e-06
NEGATIVE = -1e30
LOG2E = 1.4426950408889634
PAD = 128
ROWS = 80


def split_refs(source, count):
    wide = source.astype(jnp.float32)
    return [wide[HEAD_SIZE * h : HEAD_SIZE * (h + 1)] for h in range(count)]


def grow_rows(value, rows):
    return jnp.concatenate([value, jnp.zeros((rows - value.shape[0], value.shape[1]), value.dtype)], axis=0)


def swap_chunk(part, per, place):
    return lax.bitwise_xor(part // per, place) * per + part % per


def same_picture(kid_ref, qid_ref, key_start, query_start, block):
    key_ids = kid_ref[pl.ds(key_start, block), :]
    key_ids = jnp.concatenate([key_ids] * (block // 128), axis=1)
    return key_ids == qid_ref[0:1, pl.ds(query_start, block)]


def attend_kernel(low_ref, high_ref, place_ref, qkv_ref, kid_ref, qid_ref, out_ref, log_ref, q_t, k_n, v_t, kept, top, total, acc, *, count, block, chunk):
    step = pl.program_id(0)
    length = qkv_ref.shape[2]
    per = chunk // block
    factor = HEAD_SIZE ** (-0.5) * LOG2E

    @pl.when(step == 0)
    def _():
        @pl.loop(0, length // block)
        def _(part):
            near = pl.ds(pl.multiple_of(part * block, block), block)
            at = pl.ds(pl.multiple_of(swap_chunk(part, per, place_ref[0]) * block, block), block)
            for h, value in enumerate(split_refs(qkv_ref[0, :, near], count)):
                q_t[h, :, at] = grow_rows(value, PAD).astype(jnp.bfloat16)
            for h, value in enumerate(split_refs(qkv_ref[1, :, near], count)):
                k_n[h, at, :] = grow_rows(value, PAD).T.astype(jnp.bfloat16)
            for h, value in enumerate(split_refs(qkv_ref[2, :, near], count)):
                v_t[h, :, at] = grow_rows(value, ROWS).astype(jnp.bfloat16)

    top[...] = jnp.full(top.shape, NEGATIVE, jnp.float32)
    total[...] = jnp.zeros(total.shape, jnp.float32)
    acc[...] = jnp.zeros(acc.shape, jnp.float32)
    query_start = pl.multiple_of(step * block, block)
    queries = pl.ds(query_start, block)

    def first(index, _):
        key_start = pl.multiple_of(index * block, block)
        mask = same_picture(kid_ref, qid_ref, key_start, query_start, block)
        for h in range(count):
            scores = jnp.dot(
                k_n[h, pl.ds(key_start, block), :], q_t[h, :, queries], preferred_element_type=jnp.float32
            )
            scores = jnp.where(mask, scores * factor, NEGATIVE)
            kept[h, pl.ds(key_start, block), :] = scores
            top[h] = jnp.maximum(top[h], jnp.max(scores.reshape(block // 8, 8, block), axis=0))
        return 0

    lax.fori_loop(low_ref[step], high_ref[step], first, 0)
    highest = [jnp.max(top[h], axis=0, keepdims=True) for h in range(count)]

    def second(index, _):
        keys = pl.ds(pl.multiple_of(index * block, block), block)
        for h in range(count):
            probs = jnp.exp2(kept[h, keys, :] - highest[h])
            total[h] += jnp.sum(probs.reshape(block // 8, 8, block), axis=0)
            acc[h] += jnp.dot(v_t[h, :, keys], probs.astype(jnp.bfloat16), preferred_element_type=jnp.float32)
        return 0

    lax.fori_loop(low_ref[step], high_ref[step], second, 0)
    sums = [jnp.sum(total[h], axis=0, keepdims=True) for h in range(count)]
    for h in range(count):
        log_ref[h : h + 1, :] = highest[h] + jnp.log2(sums[h])
    out_ref[0] = jnp.concatenate([acc[h, :HEAD_SIZE] / sums[h] for h in range(count)], axis=0).astype(jnp.bfloat16)


def attend(qkv, low, high, key_ids, query_ids, place, chunk):
    _, width, length = qkv.shape
    count = width // HEAD_SIZE
    block = min(256, chunk)
    per = chunk // block
    whole = lambda *shape: pl.BlockSpec(shape, lambda i, *_: (0,) * len(shape))
    area = length * length * count // 2
    return pl.pallas_call(
        functools.partial(attend_kernel, count=count, block=block, chunk=chunk),
        name="attend",
        grid_spec=pltpu.PrefetchScalarGridSpec(
            num_scalar_prefetch=3,
            grid=(length // block,),
            in_specs=[whole(3, width, length), whole(length, 128), whole(8, length)],
            out_specs=[
                pl.BlockSpec((1, width, block), lambda i, low, high, place: (lax.bitwise_xor(i // per, place[0]), 0, i % per)),
                pl.BlockSpec((max(8, count), block), lambda i, *_: (0, i)),
            ],
            scratch_shapes=[
                pltpu.VMEM((count, PAD, length), jnp.bfloat16),
                pltpu.VMEM((count, length, PAD), jnp.bfloat16),
                pltpu.VMEM((count, ROWS, length), jnp.bfloat16),
                pltpu.VMEM((count, length, block), jnp.float32),
                pltpu.VMEM((count, 8, block), jnp.float32),
                pltpu.VMEM((count, 8, block), jnp.float32),
                pltpu.VMEM((count, ROWS, block), jnp.float32),
            ],
        ),
        out_shape=[
            jax.ShapeDtypeStruct((length // chunk, width, chunk), jnp.bfloat16),
            jax.ShapeDtypeStruct((max(8, count), length), jnp.float32),
        ],
        compiler_params=pltpu.CompilerParams(vmem_limit_bytes=40 << 20),
        cost_estimate=pl.CostEstimate(flops=area * 800, transcendentals=area, bytes_accessed=8 * length * width),
    )(low, high, place, qkv, key_ids, query_ids)


def attend_back_kernel(
    low_ref, high_ref, place_ref, qkv_ref, out_ref, log_ref, kid_ref, qid_ref, *rest, count, block, chunks,
):
    gm_refs, grad_ref = rest[:chunks], rest[chunks]
    q_t, k_t, k_n, v_n, g_t, delta, gq, gk, gv = rest[chunks + 1 :]
    step = pl.program_id(0)
    length = qkv_ref.shape[2]
    chunk = length // chunks
    per = chunk // block
    place = place_ref[0]
    scale = HEAD_SIZE ** (-0.5)
    factor = scale * LOG2E

    @pl.when(step == 0)
    def _():
        gq[...] = jnp.zeros(gq.shape, jnp.float32)

        @pl.loop(0, length // block)
        def _(part):
            near = pl.ds(pl.multiple_of(part * block, block), block)
            at = pl.ds(pl.multiple_of(swap_chunk(part, per, place) * block, block), block)
            for h, value in enumerate(split_refs(qkv_ref[0, :, near], count)):
                q_t[h, :, at] = grow_rows(value, PAD).astype(jnp.bfloat16)
            for h, value in enumerate(split_refs(qkv_ref[1, :, near], count)):
                value = grow_rows(value, PAD)
                k_t[h, :, at] = value[:ROWS].astype(jnp.bfloat16)
                k_n[h, at, :] = value.T.astype(jnp.bfloat16)
            for h, value in enumerate(split_refs(qkv_ref[2, :, near], count)):
                v_n[h, at, :] = grow_rows(value, PAD).T.astype(jnp.bfloat16)

        for piece in range(chunks):
            at = pl.ds(pl.multiple_of(lax.bitwise_xor(piece, place) * chunk, chunk), chunk)
            grads = split_refs(gm_refs[piece][...], count)
            outs = split_refs(out_ref[piece], count)
            for h in range(count):
                g_t[h, :, at] = grow_rows(grads[h], PAD).astype(jnp.bfloat16)
                delta[h, :, at] = jnp.sum(grads[h] * outs[h], axis=0, keepdims=True)

    gk[...] = jnp.zeros(gk.shape, jnp.float32)
    gv[...] = jnp.zeros(gv.shape, jnp.float32)
    key_start = pl.multiple_of(step * block, block)
    keys = pl.ds(key_start, block)

    def one(index, _):
        query_start = pl.multiple_of(index * block, block)
        queries = pl.ds(query_start, block)
        mask = same_picture(kid_ref, qid_ref, key_start, query_start, block)
        for h in range(count):
            scores = jnp.dot(k_n[h, keys, :], q_t[h, :, queries], preferred_element_type=jnp.float32)
            probs = jnp.where(mask, jnp.exp2(scores * factor - log_ref[h : h + 1, queries]), 0.0)
            back = jnp.dot(v_n[h, keys, :], g_t[h, :, queries], preferred_element_type=jnp.float32)
            slope = (probs * (back - delta[h, :, queries])).astype(jnp.bfloat16)
            nt = (((1,), (1,)), ((), ()))
            gv[h] += lax.dot_general(
                g_t[h, :ROWS, queries], probs.astype(jnp.bfloat16), nt, preferred_element_type=jnp.float32
            )
            gk[h] += lax.dot_general(q_t[h, :ROWS, queries], slope, nt, preferred_element_type=jnp.float32)
            gq[h, :, queries] += jnp.dot(k_t[h, :, keys], slope, preferred_element_type=jnp.float32)
        return 0

    lax.fori_loop(low_ref[step], high_ref[step], one, 0)
    near = pl.ds(pl.multiple_of(swap_chunk(step, per, place) * block, block), block)
    grad_ref[1, :, near] = (jnp.concatenate([gk[h, :HEAD_SIZE] for h in range(count)], axis=0) * scale).astype(jnp.bfloat16)
    grad_ref[2, :, near] = jnp.concatenate([gv[h, :HEAD_SIZE] for h in range(count)], axis=0).astype(jnp.bfloat16)

    @pl.when(step == pl.num_programs(0) - 1)
    def _():
        @pl.loop(0, length // block)
        def _(part):
            near = pl.ds(pl.multiple_of(part * block, block), block)
            at = pl.ds(pl.multiple_of(swap_chunk(part, per, place) * block, block), block)
            grad_ref[0, :, near] = (
                jnp.concatenate([gq[h, :HEAD_SIZE, at] for h in range(count)], axis=0) * scale
            ).astype(jnp.bfloat16)


def attend_back(qkv, grad_mixed, mixed, logsum, low, high, key_ids, query_ids, place):
    _, width, length = qkv.shape
    chunk = mixed.shape[2]
    count = width // HEAD_SIZE
    block = min(256, chunk)
    whole = lambda *shape: pl.BlockSpec(shape, lambda i, *_: (0,) * len(shape))
    area = length * length * count // 2
    return pl.pallas_call(
        functools.partial(attend_back_kernel, count=count, block=block, chunks=mixed.shape[0]),
        name="attend_back",
        grid_spec=pltpu.PrefetchScalarGridSpec(
            num_scalar_prefetch=3,
            grid=(length // block,),
            in_specs=[
                whole(3, width, length),
                whole(*mixed.shape),
                whole(max(8, count), length),
                whole(length, 128),
                whole(8, length),
            ]
            + [whole(*piece.shape) for piece in grad_mixed],
            out_specs=whole(3, width, length),
            scratch_shapes=[
                pltpu.VMEM((count, PAD, length), jnp.bfloat16),
                pltpu.VMEM((count, ROWS, length), jnp.bfloat16),
                pltpu.VMEM((count, length, PAD), jnp.bfloat16),
                pltpu.VMEM((count, length, PAD), jnp.bfloat16),
                pltpu.VMEM((count, PAD, length), jnp.bfloat16),
                pltpu.VMEM((count, 1, length), jnp.float32),
                pltpu.VMEM((count, ROWS, length), jnp.float32),
                pltpu.VMEM((count, ROWS, block), jnp.float32),
                pltpu.VMEM((count, ROWS, block), jnp.float32),
            ],
        ),
        out_shape=jax.ShapeDtypeStruct((3, width, length), jnp.bfloat16),
        compiler_params=pltpu.CompilerParams(vmem_limit_bytes=60 << 20),
        cost_estimate=pl.CostEstimate(flops=area * 2000, transcendentals=area, bytes_accessed=16 * length * width),
    )(low, high, place, qkv, mixed, logsum, key_ids, query_ids, *grad_mixed)


def block_ranges(ids, block):
    ids = jnp.where(ids < 0, 1 << 20, ids).reshape(-1, block)
    first, last = ids[:, 0], ids[:, -1]
    low = jnp.sum((last[None, :] < first[:, None]).astype(jnp.int32), axis=1)
    high = jnp.sum((first[None, :] <= last[:, None]).astype(jnp.int32), axis=1)
    return low, high


def norm_parts(value_rows):
    center = value_rows - jnp.mean(value_rows, axis=-1, keepdims=True)
    inverse = lax.rsqrt(jnp.mean(center * center, axis=-1, keepdims=True) + EPS)
    return center * inverse, inverse


def norm_back(grad, normed, inverse, gain):
    scaled = grad * gain
    flat = jnp.mean(scaled, axis=-1, keepdims=True)
    along = jnp.mean(scaled * normed, axis=-1, keepdims=True)
    return inverse * (scaled - flat - normed * along)


def contract(left, right, left_axis, right_axis):
    return lax.dot_general(left, right, (((left_axis,), (right_axis,)), ((), ())), preferred_element_type=jnp.float32)


def per_device(
    tokens, picture_ids, attn_gain, attn_shift, query_weight, query_bias, key_weight, value_weight, value_bias,
    output_weight, output_bias, mlp_gain, mlp_shift, up_weight, up_bias, down_weight, down_bias, cotangent,
    *, seq_count, row_count,
):
    count, chunk, width = tokens.shape
    length = chunk * seq_count
    part = width // seq_count
    band_width = width // row_count
    hidden_size = up_weight.shape[1]
    slab = -(-hidden_size // (seq_count * 128)) * 128
    place = lax.axis_index("seq")
    place_array = place.reshape(1).astype(jnp.int32)
    block = min(256, chunk)
    f32, bf16 = jnp.float32, jnp.bfloat16
    rest = range(1, seq_count)

    def swap(value, hop):
        return lax.ppermute(value, "seq", [(i, i ^ hop) for i in range(seq_count)])

    def own_columns(weight):
        return lax.dynamic_slice_in_dim(weight, place * part, part, axis=1)

    def relative(stacked):
        return [lax.dynamic_index_in_dim(stacked, place ^ hop, axis=0, keepdims=False) for hop in range(seq_count)]

    whole_rows = [[tokens[row]] for row in range(count)]
    token_rows = [tokens[row] for row in range(count)]
    for row in range(count):
        if row:
            held = lax.optimization_barrier((token_rows[row], *whole_rows[row - 1][1:]))
            token_rows[row], whole_rows[row - 1][1:] = held[0], list(held[1:])
        whole_rows[row] += [swap(token_rows[row], hop) for hop in rest]

    small = [attn_gain, attn_shift, query_bias, value_bias, output_bias, mlp_gain, mlp_shift, down_bias]
    wide = -(-up_bias.shape[0] // band_width)
    up_columns = jnp.pad(up_bias, (0, wide * band_width - up_bias.shape[0])).reshape(wide, band_width).T
    heads_shard = jnp.concatenate(
        [own_columns(query_weight), own_columns(key_weight), own_columns(value_weight), jnp.stack(small, axis=1), up_columns],
        axis=1,
    )
    gathered = lax.all_gather(heads_shard, "rows", axis=0, tiled=True)
    heads_weight = gathered[:, : 3 * part]
    extra = gathered[:, 3 * part :].astype(f32)
    gain1, shift1, query_off, value_off, output_off, gain2, shift2, down_off = [extra[:, i] for i in range(8)]
    up_off = extra[:, 8:].reshape(row_count, band_width, wide).transpose(0, 2, 1).reshape(row_count, wide * band_width)
    up_off = up_off[:, : up_bias.shape[0]].reshape(hidden_size)
    up_off = relative(jnp.pad(up_off, (0, slab * seq_count - hidden_size)).reshape(seq_count, slab))
    heads_off = jnp.concatenate(
        [
            lax.dynamic_slice_in_dim(query_off, place * part, part),
            jnp.zeros((part,), f32),
            lax.dynamic_slice_in_dim(value_off, place * part, part),
        ]
    )

    def in_slabs(weight):
        return jnp.pad(weight, ((0, 0), (0, slab * seq_count - hidden_size)))

    def own_slab(weight, hop):
        return lax.dynamic_slice_in_dim(weight, (place ^ hop) * slab, slab, axis=1)

    down_own = lax.all_gather(own_slab(in_slabs(down_weight.T), 0), "rows", axis=0, tiled=True)
    output_whole = lax.all_gather(output_weight, "rows", axis=0, tiled=True)
    near_up = jnp.concatenate([own_slab(in_slabs(up_weight), hop) for hop in range(seq_count)], axis=1)
    up_whole = lax.all_gather(near_up, "rows", axis=0, tiled=True)
    held = lax.optimization_barrier((down_own, *whole_rows[-1][1:]))
    down_own, whole_rows[-1][1:] = held[0], list(held[1:])
    downs = [down_own] + [swap(down_own, hop) for hop in rest]
    up_off = jnp.concatenate(up_off)
    outputs = relative(output_whole.reshape(seq_count, part, width))

    attn_inputs, packs, mixes, logs, tables, mixed_own = [], [], [], [], [], []
    for row in range(count):
        ids = picture_ids[row]
        low, high = block_ranges(ids, block)
        tables.append((low, high, jnp.broadcast_to(ids[:, None], (length, 128)), jnp.broadcast_to(ids[None], (8, length))))
        attn_input = jnp.concatenate(
            [(norm_parts(piece.astype(f32))[0] * gain1 + shift1).astype(bf16) for piece in whole_rows[row]], axis=0
        )
        pack = (contract(heads_weight, attn_input, 0, 1) + heads_off[:, None]).astype(bf16).reshape(3, part, length)
        mixed, logsum = attend(pack, *tables[row], place_array, chunk)
        attn_inputs.append(attn_input)
        packs.append(pack)
        mixes.append(mixed)
        logs.append(logsum)
        mixed_own.append([mixed[0]] + [swap(mixed[hop], hop) for hop in rest])

    mixed_all = jnp.concatenate(
        [jnp.concatenate([mixed_own[row][hop] for row in range(count)], axis=1) for hop in range(seq_count)], axis=0
    )
    output_near = jnp.concatenate(outputs, axis=0)
    tokens_own = tokens.reshape(count * chunk, width).astype(f32)
    resid = tokens_own + (contract(mixed_all, output_near, 0, 0) + output_off)
    normed2, inverse2 = norm_parts(resid)
    mlp_input = (normed2 * gain2 + shift2).astype(bf16)
    total = None
    hidden = contract(mlp_input, up_whole, 1, 0) + up_off
    gelu_out, pull = jax.vjp(lambda v: jax.nn.gelu(v, approximate=True), hidden)
    gelu_out, slope = gelu_out.astype(bf16), pull(jnp.ones_like(hidden))[0].astype(bf16)

    def slab_of(value, hop):
        return value[:, hop * slab : (hop + 1) * slab]

    for hop in range(seq_count):
        term = contract(slab_of(gelu_out, hop), downs[hop], 1, 1)
        total = term if total is None else total + term
    activations = resid + total + down_off

    def exchange_sum(pieces):
        total = pieces[0].astype(f32)
        for hop in rest:
            total = total + swap(pieces[hop], hop).astype(f32)
        return total

    cot = cotangent.reshape(count * chunk, width)
    grad_down = contract(cot, gelu_out, 0, 0).astype(bf16)
    cot, grad_down = lax.optimization_barrier((cot, grad_down))
    down_raw = lax.psum_scatter(grad_down, "rows", scatter_dimension=0, tiled=True)
    grad_hidden = jnp.concatenate(
        [(contract(cot, downs[hop], 1, 0) * slab_of(slope, hop).astype(f32)).astype(bf16) for hop in range(seq_count)], axis=1
    )
    grad_mlp_input = contract(grad_hidden, up_whole, 1, 1)
    grad_up = contract(mlp_input, grad_hidden, 0, 0).astype(bf16)
    grad_resid = cot.astype(f32) + norm_back(grad_mlp_input, normed2, inverse2, gain2)
    grad_attn = grad_resid.astype(bf16)

    grad_output = contract(mixed_all, grad_attn, 1, 0)
    grad_output = relative(grad_output.astype(bf16).reshape(seq_count, part, width))
    grad_output = jnp.concatenate(grad_output, axis=0)
    packs[0], down_raw, grad_up, grad_output = lax.optimization_barrier((packs[0], down_raw, grad_up, grad_output))
    up_raw = lax.psum_scatter(grad_up, "rows", scatter_dimension=0, tiled=True)
    down_share = exchange_sum([slab_of(down_raw, hop) for hop in range(seq_count)]).astype(bf16)
    heads_grad, query_grad, value_grad, gain_grad, shift_grad, grad_in = None, 0.0, 0.0, 0.0, 0.0, []
    after = None
    for row in range(count):
        grad_mixed = []
        for hop in range(seq_count):
            piece = contract(outputs[hop], grad_attn[row * chunk : (row + 1) * chunk], 1, 1).astype(bf16)
            grad_mixed.append(swap(piece, hop) if hop else piece)
        pack = packs[row]
        if after is not None:
            pack, grad_in[-1] = lax.optimization_barrier((pack, grad_in[-1]))
        grad_pack = attend_back(pack, grad_mixed, mixes[row], logs[row], *tables[row], place_array)
        if row == count - 1:
            grad_pack, up_raw, grad_output = lax.optimization_barrier((grad_pack, up_raw, grad_output))
            output_share = lax.psum_scatter(grad_output, "rows", scatter_dimension=0, tiled=True)
            up_share = exchange_sum([slab_of(up_raw, hop) for hop in range(seq_count)]).astype(bf16)
        query_grad = query_grad + jnp.sum(grad_pack[0].astype(f32), axis=1)
        value_grad = value_grad + jnp.sum(grad_pack[2].astype(f32), axis=1)
        grad_pack = grad_pack.reshape(3 * part, length)
        partial = []
        for hop in range(seq_count):
            piece = contract(grad_pack[:, hop * chunk : (hop + 1) * chunk], heads_weight, 0, 1)
            gain_grad = gain_grad + jnp.sum(piece * norm_parts(whole_rows[row][hop].astype(f32))[0], axis=0)
            shift_grad = shift_grad + jnp.sum(piece, axis=0)
            partial.append(piece.astype(bf16))
        grad_in.append(partial)
        after = partial
        term = contract(attn_inputs[row], grad_pack, 0, 1)
        heads_grad = term if heads_grad is None else heads_grad + term

    def placed(value):
        return lax.dynamic_update_slice_in_dim(jnp.zeros((width,), f32), value, place * part, axis=0)

    up_grads = jnp.stack(relative(jnp.sum(grad_hidden.astype(f32), axis=0).reshape(seq_count, slab)))
    small_grads = [
        gain_grad,
        shift_grad,
        placed(query_grad),
        placed(value_grad),
        jnp.sum(grad_attn.astype(f32), axis=0),
        jnp.sum(grad_mlp_input * normed2, axis=0),
        jnp.sum(grad_mlp_input, axis=0),
        jnp.sum(cot.astype(f32), axis=0),
        up_grads.reshape(slab * seq_count)[:hidden_size],
    ]
    together = jnp.concatenate([value.reshape(row_count, -1) for value in small_grads], axis=1)
    sizes = [value.shape[0] // row_count for value in small_grads]
    filled = -(-together.shape[1] // 2048) * 2048
    together = jnp.pad(together, ((0, 0), (0, filled - together.shape[1]))).reshape(row_count * filled // 128, 128)
    heads_grad = heads_grad.astype(bf16)
    heads_grad, output_share = lax.optimization_barrier((heads_grad, output_share))
    heads_share = lax.psum_scatter(heads_grad, "rows", scatter_dimension=0, tiled=True)
    together, heads_share = lax.optimization_barrier((together, heads_share))
    small_share = lax.psum_scatter(together, "rows", scatter_dimension=0, tiled=True)

    normed1, inverse1 = norm_parts(tokens_own)
    sums = []
    for row in range(count):
        sums.append(exchange_sum(grad_in[row]))
    grad_attn_input = jnp.concatenate(sums, axis=0)
    token_grad = grad_resid + norm_back(grad_attn_input, normed1, inverse1, gain1)

    def all_pieces(share):
        stacked = jnp.stack([share] + [swap(share, hop) for hop in rest])
        return relative(stacked)

    def seq_sum(share):
        total = share.astype(f32)
        for hop in rest:
            total = total + swap(share, hop).astype(f32)
        return total

    heads_all = [piece.astype(f32) for piece in all_pieces(heads_share)]
    small_sum = seq_sum(small_share).reshape(-1)
    vectors, start = [], 0
    for size in sizes:
        vectors.append(small_sum[start : start + size])
        start += size

    def take(which):
        return jnp.concatenate([piece[:, which * part : (which + 1) * part] for piece in heads_all], axis=1)

    def slabs(share):
        return jnp.concatenate([piece.astype(f32) for piece in all_pieces(share)], axis=1)[:, :hidden_size]

    return (
        activations.reshape(count, chunk, width),
        token_grad.reshape(count, chunk, width),
        vectors[0],
        vectors[1],
        take(0),
        vectors[2],
        take(1),
        take(2),
        vectors[3],
        seq_sum(output_share),
        vectors[4],
        vectors[5],
        vectors[6],
        slabs(up_share),
        vectors[8],
        slabs(down_share).T,
        vectors[7],
    )


def solution(mesh):
    matrix, vector, batch = P("rows", None), P("rows"), P("rows", "seq", None)
    columns = P(None, "rows")

    def body(*arguments):
        return per_device(*arguments, seq_count=mesh.shape["seq"], row_count=mesh.shape["rows"])

    return jax.shard_map(
        body,
        mesh=mesh,
        in_specs=(
            batch, matrix, vector, vector, matrix, vector, matrix, matrix, vector, matrix, vector, vector, vector, matrix,
            vector, columns, vector, batch,
        ),
        out_specs=(
            batch, batch, vector, vector, matrix, vector, matrix, matrix, vector, matrix, vector, vector, vector, matrix,
            vector, columns, vector,
        ),
        check_vma=False,
    )
```

```python
import functools
import jax
import jax.numpy as jnp
from jax import lax
from jax.experimental import pallas as pl
from jax.experimental.layout import Layout, with_layout_constraint
from jax.experimental.pallas import tpu as pltpu
from jax.sharding import PartitionSpec as P


HEAD_SIZE = 72
EPS = 1e-06
NEGATIVE = -1e30
LOG2E = 1.4426950408889634
PAD = 128
ROWS = 80


def split_refs(source, count):
    wide = source.astype(jnp.float32)
    return [wide[HEAD_SIZE * h : HEAD_SIZE * (h + 1)] for h in range(count)]


def grow_rows(value, rows):
    return jnp.concatenate([value, jnp.zeros((rows - value.shape[0], value.shape[1]), value.dtype)], axis=0)


def swap_chunk(part, per, place):
    return lax.bitwise_xor(part // per, place) * per + part % per


def same_picture(kid_ref, qid_ref, key_start, query_start, block):
    key_ids = kid_ref[pl.ds(key_start, block), :]
    key_ids = jnp.concatenate([key_ids] * (block // 128), axis=1)
    return key_ids == qid_ref[0:1, pl.ds(query_start, block)]


def attend_kernel(low_ref, high_ref, place_ref, qkv_ref, kid_ref, qid_ref, out_ref, log_ref, q_t, k_n, v_t, kept, top, total, acc, *, count, block, chunk):
    step = pl.program_id(0)
    length = qkv_ref.shape[2]
    per = chunk // block
    factor = HEAD_SIZE ** (-0.5) * LOG2E

    @pl.when(step == 0)
    def _():
        @pl.loop(0, length // block)
        def _(part):
            near = pl.ds(pl.multiple_of(part * block, block), block)
            at = pl.ds(pl.multiple_of(swap_chunk(part, per, place_ref[0]) * block, block), block)
            for h, value in enumerate(split_refs(qkv_ref[0, :, near], count)):
                q_t[h, :, at] = grow_rows(value, PAD).astype(jnp.bfloat16)
            for h, value in enumerate(split_refs(qkv_ref[1, :, near], count)):
                k_n[h, at, :] = grow_rows(value, PAD).T.astype(jnp.bfloat16)
            for h, value in enumerate(split_refs(qkv_ref[2, :, near], count)):
                v_t[h, :, at] = grow_rows(value, ROWS).astype(jnp.bfloat16)

    top[...] = jnp.full(top.shape, NEGATIVE, jnp.float32)
    total[...] = jnp.zeros(total.shape, jnp.float32)
    acc[...] = jnp.zeros(acc.shape, jnp.float32)
    query_start = pl.multiple_of(step * block, block)
    queries = pl.ds(query_start, block)

    def first(index, _):
        key_start = pl.multiple_of(index * block, block)
        mask = same_picture(kid_ref, qid_ref, key_start, query_start, block)
        for h in range(count):
            scores = jnp.dot(
                k_n[h, pl.ds(key_start, block), :], q_t[h, :, queries], preferred_element_type=jnp.float32
            )
            scores = jnp.where(mask, scores * factor, NEGATIVE)
            kept[h, pl.ds(key_start, block), :] = scores
            top[h] = jnp.maximum(top[h], jnp.max(scores.reshape(block // 8, 8, block), axis=0))
        return 0

    lax.fori_loop(low_ref[step], high_ref[step], first, 0)
    highest = [jnp.max(top[h], axis=0, keepdims=True) for h in range(count)]

    def second(index, _):
        keys = pl.ds(pl.multiple_of(index * block, block), block)
        for h in range(count):
            probs = jnp.exp2(kept[h, keys, :] - highest[h])
            total[h] += jnp.sum(probs.reshape(block // 8, 8, block), axis=0)
            acc[h] += jnp.dot(v_t[h, :, keys], probs.astype(jnp.bfloat16), preferred_element_type=jnp.float32)
        return 0

    lax.fori_loop(low_ref[step], high_ref[step], second, 0)
    sums = [jnp.sum(total[h], axis=0, keepdims=True) for h in range(count)]
    for h in range(count):
        log_ref[h : h + 1, :] = highest[h] + jnp.log2(sums[h])
    out_ref[0] = jnp.concatenate([acc[h, :HEAD_SIZE] / sums[h] for h in range(count)], axis=0).astype(jnp.bfloat16)


def attend(qkv, low, high, key_ids, query_ids, place, chunk):
    _, width, length = qkv.shape
    count = width // HEAD_SIZE
    block = min(256, chunk)
    per = chunk // block
    whole = lambda *shape: pl.BlockSpec(shape, lambda i, *_: (0,) * len(shape))
    area = length * length * count // 2
    return pl.pallas_call(
        functools.partial(attend_kernel, count=count, block=block, chunk=chunk),
        name="attend",
        grid_spec=pltpu.PrefetchScalarGridSpec(
            num_scalar_prefetch=3,
            grid=(length // block,),
            in_specs=[whole(3, width, length), whole(length, 128), whole(8, length)],
            out_specs=[
                pl.BlockSpec((1, width, block), lambda i, low, high, place: (lax.bitwise_xor(i // per, place[0]), 0, i % per)),
                pl.BlockSpec((max(8, count), block), lambda i, *_: (0, i)),
            ],
            scratch_shapes=[
                pltpu.VMEM((count, PAD, length), jnp.bfloat16),
                pltpu.VMEM((count, length, PAD), jnp.bfloat16),
                pltpu.VMEM((count, ROWS, length), jnp.bfloat16),
                pltpu.VMEM((count, length, block), jnp.float32),
                pltpu.VMEM((count, 8, block), jnp.float32),
                pltpu.VMEM((count, 8, block), jnp.float32),
                pltpu.VMEM((count, ROWS, block), jnp.float32),
            ],
        ),
        out_shape=[
            jax.ShapeDtypeStruct((length // chunk, width, chunk), jnp.bfloat16),
            jax.ShapeDtypeStruct((max(8, count), length), jnp.float32),
        ],
        compiler_params=pltpu.CompilerParams(vmem_limit_bytes=40 << 20),
        cost_estimate=pl.CostEstimate(flops=area * 800, transcendentals=area, bytes_accessed=8 * length * width),
    )(low, high, place, qkv, key_ids, query_ids)


def attend_back_kernel(
    low_ref, high_ref, place_ref, qkv_ref, out_ref, log_ref, kid_ref, qid_ref, *rest, count, block, chunks,
):
    gm_refs, grad_ref = rest[:chunks], rest[chunks]
    q_t, k_t, k_n, v_n, g_t, delta, gq, gk, gv = rest[chunks + 1 :]
    step = pl.program_id(0)
    length = qkv_ref.shape[2]
    chunk = length // chunks
    per = chunk // block
    place = place_ref[0]
    scale = HEAD_SIZE ** (-0.5)
    factor = scale * LOG2E

    @pl.when(step == 0)
    def _():
        gq[...] = jnp.zeros(gq.shape, jnp.float32)

        @pl.loop(0, length // block)
        def _(part):
            near = pl.ds(pl.multiple_of(part * block, block), block)
            at = pl.ds(pl.multiple_of(swap_chunk(part, per, place) * block, block), block)
            for h, value in enumerate(split_refs(qkv_ref[0, :, near], count)):
                q_t[h, :, at] = grow_rows(value, PAD).astype(jnp.bfloat16)
            for h, value in enumerate(split_refs(qkv_ref[1, :, near], count)):
                value = grow_rows(value, PAD)
                k_t[h, :, at] = value[:ROWS].astype(jnp.bfloat16)
                k_n[h, at, :] = value.T.astype(jnp.bfloat16)
            for h, value in enumerate(split_refs(qkv_ref[2, :, near], count)):
                v_n[h, at, :] = grow_rows(value, PAD).T.astype(jnp.bfloat16)

        for piece in range(chunks):
            at = pl.ds(pl.multiple_of(lax.bitwise_xor(piece, place) * chunk, chunk), chunk)
            grads = split_refs(gm_refs[piece][...], count)
            outs = split_refs(out_ref[piece], count)
            for h in range(count):
                g_t[h, :, at] = grow_rows(grads[h], PAD).astype(jnp.bfloat16)
                delta[h, :, at] = jnp.sum(grads[h] * outs[h], axis=0, keepdims=True)

    gk[...] = jnp.zeros(gk.shape, jnp.float32)
    gv[...] = jnp.zeros(gv.shape, jnp.float32)
    key_start = pl.multiple_of(step * block, block)
    keys = pl.ds(key_start, block)

    def one(index, _):
        query_start = pl.multiple_of(index * block, block)
        queries = pl.ds(query_start, block)
        mask = same_picture(kid_ref, qid_ref, key_start, query_start, block)
        for h in range(count):
            scores = jnp.dot(k_n[h, keys, :], q_t[h, :, queries], preferred_element_type=jnp.float32)
            probs = jnp.where(mask, jnp.exp2(scores * factor - log_ref[h : h + 1, queries]), 0.0)
            back = jnp.dot(v_n[h, keys, :], g_t[h, :, queries], preferred_element_type=jnp.float32)
            slope = (probs * (back - delta[h, :, queries])).astype(jnp.bfloat16)
            nt = (((1,), (1,)), ((), ()))
            gv[h] += lax.dot_general(
                g_t[h, :ROWS, queries], probs.astype(jnp.bfloat16), nt, preferred_element_type=jnp.float32
            )
            gk[h] += lax.dot_general(q_t[h, :ROWS, queries], slope, nt, preferred_element_type=jnp.float32)
            gq[h, :, queries] += jnp.dot(k_t[h, :, keys], slope, preferred_element_type=jnp.float32)
        return 0

    lax.fori_loop(low_ref[step], high_ref[step], one, 0)
    near = pl.ds(pl.multiple_of(swap_chunk(step, per, place) * block, block), block)
    grad_ref[1, :, near] = (jnp.concatenate([gk[h, :HEAD_SIZE] for h in range(count)], axis=0) * scale).astype(jnp.bfloat16)
    grad_ref[2, :, near] = jnp.concatenate([gv[h, :HEAD_SIZE] for h in range(count)], axis=0).astype(jnp.bfloat16)

    @pl.when(step == pl.num_programs(0) - 1)
    def _():
        @pl.loop(0, length // block)
        def _(part):
            near = pl.ds(pl.multiple_of(part * block, block), block)
            at = pl.ds(pl.multiple_of(swap_chunk(part, per, place) * block, block), block)
            grad_ref[0, :, near] = (
                jnp.concatenate([gq[h, :HEAD_SIZE, at] for h in range(count)], axis=0) * scale
            ).astype(jnp.bfloat16)


def attend_back(qkv, grad_mixed, mixed, logsum, low, high, key_ids, query_ids, place):
    _, width, length = qkv.shape
    chunk = mixed.shape[2]
    count = width // HEAD_SIZE
    block = min(256, chunk)
    whole = lambda *shape: pl.BlockSpec(shape, lambda i, *_: (0,) * len(shape))
    area = length * length * count // 2
    return pl.pallas_call(
        functools.partial(attend_back_kernel, count=count, block=block, chunks=mixed.shape[0]),
        name="attend_back",
        grid_spec=pltpu.PrefetchScalarGridSpec(
            num_scalar_prefetch=3,
            grid=(length // block,),
            in_specs=[
                whole(3, width, length),
                whole(*mixed.shape),
                whole(max(8, count), length),
                whole(length, 128),
                whole(8, length),
            ]
            + [whole(*piece.shape) for piece in grad_mixed],
            out_specs=whole(3, width, length),
            scratch_shapes=[
                pltpu.VMEM((count, PAD, length), jnp.bfloat16),
                pltpu.VMEM((count, ROWS, length), jnp.bfloat16),
                pltpu.VMEM((count, length, PAD), jnp.bfloat16),
                pltpu.VMEM((count, length, PAD), jnp.bfloat16),
                pltpu.VMEM((count, PAD, length), jnp.bfloat16),
                pltpu.VMEM((count, 1, length), jnp.float32),
                pltpu.VMEM((count, ROWS, length), jnp.float32),
                pltpu.VMEM((count, ROWS, block), jnp.float32),
                pltpu.VMEM((count, ROWS, block), jnp.float32),
            ],
        ),
        out_shape=jax.ShapeDtypeStruct((3, width, length), jnp.bfloat16),
        compiler_params=pltpu.CompilerParams(vmem_limit_bytes=60 << 20),
        cost_estimate=pl.CostEstimate(flops=area * 2000, transcendentals=area, bytes_accessed=16 * length * width),
    )(low, high, place, qkv, mixed, logsum, key_ids, query_ids, *grad_mixed)


def block_ranges(ids, block):
    ids = jnp.where(ids < 0, 1 << 20, ids).reshape(-1, block)
    first, last = ids[:, 0], ids[:, -1]
    low = jnp.sum((last[None, :] < first[:, None]).astype(jnp.int32), axis=1)
    high = jnp.sum((first[None, :] <= last[:, None]).astype(jnp.int32), axis=1)
    return low, high


def norm_parts(value_rows):
    center = value_rows - jnp.mean(value_rows, axis=-1, keepdims=True)
    inverse = lax.rsqrt(jnp.mean(center * center, axis=-1, keepdims=True) + EPS)
    return center * inverse, inverse


def norm_back(grad, normed, inverse, gain):
    scaled = grad * gain
    flat = jnp.mean(scaled, axis=-1, keepdims=True)
    along = jnp.mean(scaled * normed, axis=-1, keepdims=True)
    return inverse * (scaled - flat - normed * along)


def contract(left, right, left_axis, right_axis):
    return lax.dot_general(left, right, (((left_axis,), (right_axis,)), ((), ())), preferred_element_type=jnp.float32)


def per_device(
    tokens, picture_ids, attn_gain, attn_shift, query_weight, query_bias, key_weight, value_weight, value_bias,
    output_weight, output_bias, mlp_gain, mlp_shift, up_weight, up_bias, down_weight, down_bias, cotangent,
    *, seq_count, row_count,
):
    count, chunk, width = tokens.shape
    length = chunk * seq_count
    part = width // seq_count
    band_width = width // row_count
    hidden_size = up_weight.shape[1]
    slab = -(-hidden_size // (seq_count * 128)) * 128
    place = lax.axis_index("seq")
    place_array = place.reshape(1).astype(jnp.int32)
    block = min(256, chunk)
    f32, bf16 = jnp.float32, jnp.bfloat16
    rest = range(1, seq_count)

    def swap(value, hop):
        return lax.ppermute(value, "seq", [(i, i ^ hop) for i in range(seq_count)])

    def own_columns(weight):
        return lax.dynamic_slice_in_dim(weight, place * part, part, axis=1)

    def relative(stacked):
        return [lax.dynamic_index_in_dim(stacked, place ^ hop, axis=0, keepdims=False) for hop in range(seq_count)]

    whole_rows = [[tokens[row]] for row in range(count)]
    token_rows = [tokens[row] for row in range(count)]
    for row in range(count):
        if row:
            held = lax.optimization_barrier((token_rows[row], *whole_rows[row - 1][1:]))
            token_rows[row], whole_rows[row - 1][1:] = held[0], list(held[1:])
        whole_rows[row] += [swap(token_rows[row], hop) for hop in rest]

    small = [attn_gain, attn_shift, query_bias, value_bias, output_bias, mlp_gain, mlp_shift, down_bias, up_bias]
    sizes = [value.shape[0] for value in small]
    extra_rows = -(-sum(sizes) // (24 * part)) * 8

    def beside(matrix, vectors):
        lead = vectors.shape[:-1]
        vectors = jnp.pad(vectors, [(0, 0)] * len(lead) + [(0, extra_rows * 3 * part - vectors.shape[-1])])
        return jnp.concatenate([matrix, vectors.reshape(*lead, extra_rows, 3 * part)], axis=-2)

    def split(vectors):
        pieces, start = [], 0
        for size in sizes:
            pieces.append(vectors[..., start : start + size])
            start += size
        return pieces

    heads_shard = jnp.concatenate([own_columns(query_weight), own_columns(key_weight), own_columns(value_weight)], axis=1)
    heads_shard = beside(heads_shard, jnp.concatenate(small))
    gathered = lax.all_gather(heads_shard, "rows", axis=0, tiled=False)
    heads_weight = gathered[:, :band_width].reshape(width, 3 * part)
    extra = gathered[:, band_width:].reshape(row_count, extra_rows * 3 * part).astype(f32)
    gain1, shift1, query_off, value_off, output_off, gain2, shift2, down_off, up_off = [
        piece.reshape(-1) for piece in split(extra)
    ]
    up_off = relative(jnp.pad(up_off, (0, slab * seq_count - hidden_size)).reshape(seq_count, slab))
    heads_off = jnp.concatenate(
        [
            lax.dynamic_slice_in_dim(query_off, place * part, part),
            jnp.zeros((part,), f32),
            lax.dynamic_slice_in_dim(value_off, place * part, part),
        ]
    )

    def in_slabs(weight):
        return jnp.pad(weight, ((0, 0), (0, slab * seq_count - hidden_size)))

    def own_slab(weight, hop):
        return lax.dynamic_slice_in_dim(weight, (place ^ hop) * slab, slab, axis=1)

    def near_slabs(weight, hops):
        weight = in_slabs(weight)
        return lax.all_gather(jnp.concatenate([own_slab(weight, hop) for hop in hops], axis=1), "rows", axis=0, tiled=True)

    direct = list(rest)[:2]
    down_turned = down_weight.T
    down_own = near_slabs(down_turned, [0])
    output_whole = lax.all_gather(output_weight, "rows", axis=0, tiled=True)
    up_whole = near_slabs(up_weight, range(seq_count))
    late = [hop for hop in rest if hop not in direct]
    held = lax.optimization_barrier((down_own, *whole_rows[-1][1:]))
    down_own, whole_rows[-1][1:] = held[0], list(held[1:])
    downs = [down_own] + [swap(down_own, hop) for hop in direct]
    if late:
        down_turned, up_whole = lax.optimization_barrier((down_turned, up_whole))
        down_late = near_slabs(down_turned, late)
        downs += [down_late[:, i * slab : (i + 1) * slab] for i in range(len(late))]
    up_off = jnp.concatenate(up_off)
    outputs = relative(output_whole.reshape(seq_count, part, width))

    attn_inputs, packs, mixes, logs, tables, mixed_own = [], [], [], [], [], []
    for row in range(count):
        ids = picture_ids[row]
        low, high = block_ranges(ids, block)
        tables.append((low, high, jnp.broadcast_to(ids[:, None], (length, 128)), jnp.broadcast_to(ids[None], (8, length))))
        attn_input = jnp.concatenate(
            [(norm_parts(piece.astype(f32))[0] * gain1 + shift1).astype(bf16) for piece in whole_rows[row]], axis=0
        )
        pack = (contract(heads_weight, attn_input, 0, 1) + heads_off[:, None]).astype(bf16).reshape(3, part, length)
        mixed, logsum = attend(pack, *tables[row], place_array, chunk)
        attn_inputs.append(attn_input)
        packs.append(pack)
        mixes.append(mixed)
        logs.append(logsum)
        mixed_own.append([mixed[0]] + [swap(mixed[hop], hop) for hop in rest])

    mixed_all = jnp.concatenate(
        [jnp.concatenate([mixed_own[row][hop] for row in range(count)], axis=1) for hop in range(seq_count)], axis=0
    )
    output_near = jnp.concatenate(outputs, axis=0)
    tokens_own = tokens.reshape(count * chunk, width).astype(f32)
    resid = tokens_own + (contract(mixed_all, output_near, 0, 0) + output_off)
    normed2, inverse2 = norm_parts(resid)
    mlp_input = (normed2 * gain2 + shift2).astype(bf16)
    total = None
    hidden = contract(mlp_input, up_whole, 1, 0) + up_off
    gelu_out, pull = jax.vjp(lambda v: jax.nn.gelu(v, approximate=True), hidden)
    gelu_out, slope = gelu_out.astype(bf16), pull(jnp.ones_like(hidden))[0].astype(bf16)

    def slab_of(value, hop):
        return value[:, hop * slab : (hop + 1) * slab]

    def all_pieces(share):
        stacked = jnp.stack([share] + [swap(share, hop) for hop in rest])
        return relative(stacked)

    def exchange_sum(pieces):
        total = pieces[0].astype(f32)
        for hop in rest:
            total = total + swap(pieces[hop], hop).astype(f32)
        return total

    cot = cotangent.reshape(count * chunk, width)
    grad_down = with_layout_constraint(contract(cot, gelu_out, 0, 0).astype(bf16), Layout(major_to_minor=(0, 1)))
    cot, grad_down = lax.optimization_barrier((cot, grad_down))
    down_raw = lax.psum_scatter(grad_down, "rows", scatter_dimension=0, tiled=True)
    grad_hidden = jnp.concatenate(
        [(contract(cot, downs[hop], 1, 0) * slab_of(slope, hop).astype(f32)).astype(bf16) for hop in range(seq_count)], axis=1
    )
    grad_mlp_input = contract(grad_hidden, up_whole, 1, 1)
    grad_up = contract(mlp_input, grad_hidden, 0, 0).astype(bf16)
    grad_resid = cot.astype(f32) + norm_back(grad_mlp_input, normed2, inverse2, gain2)
    grad_attn = grad_resid.astype(bf16)

    grad_output = contract(mixed_all, grad_attn, 1, 0)
    grad_output = relative(grad_output.astype(bf16).reshape(seq_count, part, width))
    grad_output = jnp.concatenate(grad_output, axis=0)
    packs[0], down_raw, grad_output = lax.optimization_barrier((packs[0], down_raw, grad_output))
    output_share = lax.psum_scatter(grad_output, "rows", scatter_dimension=0, tiled=True)
    down_share = exchange_sum([slab_of(down_raw, hop) for hop in range(seq_count)]).astype(bf16)
    down_pieces = all_pieces(down_share)
    heads_grad, query_grad, value_grad, gain_grad, shift_grad, grad_in = None, 0.0, 0.0, 0.0, 0.0, []
    after = None
    for row in range(count):
        grad_mixed = []
        for hop in range(seq_count):
            piece = contract(outputs[hop], grad_attn[row * chunk : (row + 1) * chunk], 1, 1).astype(bf16)
            grad_mixed.append(swap(piece, hop) if hop else piece)
        pack = packs[row]
        if after is not None:
            pack, grad_in[-1] = lax.optimization_barrier((pack, grad_in[-1]))
        grad_pack = attend_back(pack, grad_mixed, mixes[row], logs[row], *tables[row], place_array)
        if row == 0:
            grad_pack, output_share, grad_up = lax.optimization_barrier((grad_pack, output_share, grad_up))
            up_raw = lax.psum_scatter(grad_up, "rows", scatter_dimension=0, tiled=True)
        query_grad = query_grad + jnp.sum(grad_pack[0].astype(f32), axis=1)
        value_grad = value_grad + jnp.sum(grad_pack[2].astype(f32), axis=1)
        grad_pack = grad_pack.reshape(3 * part, length)
        partial = []
        for hop in range(seq_count):
            piece = contract(grad_pack[:, hop * chunk : (hop + 1) * chunk], heads_weight, 0, 1)
            gain_grad = gain_grad + jnp.sum(piece * norm_parts(whole_rows[row][hop].astype(f32))[0], axis=0)
            shift_grad = shift_grad + jnp.sum(piece, axis=0)
            partial.append(piece.astype(bf16))
        grad_in.append(partial)
        after = partial
        term = contract(attn_inputs[row], grad_pack, 0, 1)
        heads_grad = term if heads_grad is None else heads_grad + term

    def placed(value):
        return lax.dynamic_update_slice_in_dim(jnp.zeros((width,), f32), value, place * part, axis=0)

    up_grads = jnp.stack(relative(jnp.sum(grad_hidden.astype(f32), axis=0).reshape(seq_count, slab)))
    small_grads = [
        gain_grad,
        shift_grad,
        placed(query_grad),
        placed(value_grad),
        jnp.sum(grad_attn.astype(f32), axis=0),
        jnp.sum(grad_mlp_input * normed2, axis=0),
        jnp.sum(grad_mlp_input, axis=0),
        jnp.sum(cot.astype(f32), axis=0),
        up_grads.reshape(slab * seq_count)[:hidden_size],
    ]
    together = jnp.concatenate([value.reshape(row_count, -1) for value in small_grads], axis=1).astype(bf16)
    heads_grad = beside(heads_grad.astype(bf16).reshape(row_count, band_width, 3 * part), together)
    heads_grad, up_raw = lax.optimization_barrier((heads_grad, up_raw))
    gelu_late, output_share, up_raw, heads_grad = lax.optimization_barrier((gelu_out, output_share, up_raw, heads_grad))
    total = resid
    for hop in range(seq_count):
        total = total + contract(slab_of(gelu_late, hop), downs[hop], 1, 1)
    activations = total + down_off
    up_share = exchange_sum([slab_of(up_raw, hop) for hop in range(seq_count)]).astype(bf16)

    heads_share = lax.psum_scatter(heads_grad, "rows", scatter_dimension=0, tiled=False)
    normed1, inverse1 = norm_parts(tokens_own)
    sums = []
    for row in range(count):
        sums.append(exchange_sum(grad_in[row]))
    grad_attn_input = jnp.concatenate(sums, axis=0)
    token_grad = grad_resid + norm_back(grad_attn_input, normed1, inverse1, gain1)

    def seq_sum(share):
        total = share.astype(f32)
        for hop in rest:
            total = total + swap(share, hop).astype(f32)
        return total

    heads_all = [piece.astype(f32) for piece in all_pieces(heads_share)]
    small_sum = sum(piece[band_width:] for piece in heads_all).reshape(extra_rows * 3 * part)
    vectors = split(small_sum)

    def take(which):
        return jnp.concatenate([piece[:band_width, which * part : (which + 1) * part] for piece in heads_all], axis=1)

    def slabs(pieces):
        return jnp.concatenate([piece.astype(f32) for piece in pieces], axis=1)[:, :hidden_size]

    return (
        activations.reshape(count, chunk, width),
        token_grad.reshape(count, chunk, width),
        vectors[0],
        vectors[1],
        take(0),
        vectors[2],
        take(1),
        take(2),
        vectors[3],
        seq_sum(output_share),
        vectors[4],
        vectors[5],
        vectors[6],
        slabs(all_pieces(up_share)),
        vectors[8],
        slabs(down_pieces).T,
        vectors[7],
    )


def solution(mesh):
    matrix, vector, batch = P("rows", None), P("rows"), P("rows", "seq", None)
    columns = P(None, "rows")

    def body(*arguments):
        return per_device(*arguments, seq_count=mesh.shape["seq"], row_count=mesh.shape["rows"])

    return jax.shard_map(
        body,
        mesh=mesh,
        in_specs=(
            batch, matrix, vector, vector, matrix, vector, matrix, matrix, vector, matrix, vector, vector, vector, matrix,
            vector, columns, vector, batch,
        ),
        out_specs=(
            batch, batch, vector, vector, matrix, vector, matrix, matrix, vector, matrix, vector, vector, vector, matrix,
            vector, columns, vector,
        ),
        check_vma=False,
    )
```

```python
import functools
import math

import jax
import jax.numpy as jnp
from jax import lax
from jax.experimental import pallas as pl
from jax.experimental.layout import Layout, with_layout_constraint
from jax.experimental.pallas import tpu as pltpu
from jax.sharding import PartitionSpec as P


HEAD_SIZE = 72
EPS = 1e-06
NEGATIVE = -1e30
LOG2E = 1.4426950408889634
PAD = 128
ROWS = 80


def split_refs(source, count):
    wide = source.astype(jnp.float32)
    return [wide[HEAD_SIZE * h : HEAD_SIZE * (h + 1)] for h in range(count)]


def grow_rows(value, rows):
    return jnp.concatenate([value, jnp.zeros((rows - value.shape[0], value.shape[1]), value.dtype)], axis=0)


def swap_chunk(part, per, place):
    return lax.bitwise_xor(part // per, place) * per + part % per


def same_picture(kid_ref, qid_ref, key_start, query_start, block):
    key_ids = kid_ref[pl.ds(key_start, block), :]
    key_ids = jnp.concatenate([key_ids] * (block // 128), axis=1)
    return key_ids == qid_ref[0:1, pl.ds(query_start, block)]


def attend_kernel(low_ref, high_ref, place_ref, qkv_ref, kid_ref, qid_ref, out_ref, log_ref, q_t, k_n, v_t, kept, top, total, acc, *, count, block, chunk):
    step = pl.program_id(0)
    length = qkv_ref.shape[2]
    per = chunk // block
    factor = HEAD_SIZE ** (-0.5) * LOG2E

    @pl.when(step == 0)
    def _():
        @pl.loop(0, length // block)
        def _(part):
            near = pl.ds(pl.multiple_of(part * block, block), block)
            at = pl.ds(pl.multiple_of(swap_chunk(part, per, place_ref[0]) * block, block), block)
            for h, value in enumerate(split_refs(qkv_ref[0, :, near], count)):
                q_t[h, :, at] = grow_rows(value, PAD).astype(jnp.bfloat16)
            for h, value in enumerate(split_refs(qkv_ref[1, :, near], count)):
                k_n[h, at, :] = grow_rows(value, PAD).T.astype(jnp.bfloat16)
            for h, value in enumerate(split_refs(qkv_ref[2, :, near], count)):
                v_t[h, :, at] = grow_rows(value, ROWS).astype(jnp.bfloat16)

    top[...] = jnp.full(top.shape, NEGATIVE, jnp.float32)
    total[...] = jnp.zeros(total.shape, jnp.float32)
    acc[...] = jnp.zeros(acc.shape, jnp.float32)
    query_start = pl.multiple_of(step * block, block)
    queries = pl.ds(query_start, block)

    def first(index, _):
        key_start = pl.multiple_of(index * block, block)
        mask = same_picture(kid_ref, qid_ref, key_start, query_start, block)
        for h in range(count):
            scores = jnp.dot(
                k_n[h, pl.ds(key_start, block), :], q_t[h, :, queries], preferred_element_type=jnp.float32
            )
            scores = jnp.where(mask, scores * factor, NEGATIVE)
            kept[h, pl.ds(key_start, block), :] = scores
            top[h] = jnp.maximum(top[h], jnp.max(scores.reshape(block // 8, 8, block), axis=0))
        return 0

    lax.fori_loop(low_ref[step], high_ref[step], first, 0)
    highest = [jnp.max(top[h], axis=0, keepdims=True) for h in range(count)]

    def second(index, _):
        keys = pl.ds(pl.multiple_of(index * block, block), block)
        for h in range(count):
            probs = jnp.exp2(kept[h, keys, :] - highest[h])
            total[h] += jnp.sum(probs.reshape(block // 8, 8, block), axis=0)
            acc[h] += jnp.dot(v_t[h, :, keys], probs.astype(jnp.bfloat16), preferred_element_type=jnp.float32)
        return 0

    lax.fori_loop(low_ref[step], high_ref[step], second, 0)
    sums = [jnp.sum(total[h], axis=0, keepdims=True) for h in range(count)]
    for h in range(count):
        log_ref[h : h + 1, :] = highest[h] + jnp.log2(sums[h])
    out_ref[0] = jnp.concatenate([acc[h, :HEAD_SIZE] / sums[h] for h in range(count)], axis=0).astype(jnp.bfloat16)


def attend(qkv, low, high, key_ids, query_ids, place, chunk):
    _, width, length = qkv.shape
    count = width // HEAD_SIZE
    block = min(256, chunk)
    per = chunk // block
    whole = lambda *shape: pl.BlockSpec(shape, lambda i, *_: (0,) * len(shape))
    area = length * length * count // 2
    return pl.pallas_call(
        functools.partial(attend_kernel, count=count, block=block, chunk=chunk),
        name="attend",
        grid_spec=pltpu.PrefetchScalarGridSpec(
            num_scalar_prefetch=3,
            grid=(length // block,),
            in_specs=[whole(3, width, length), whole(length, 128), whole(8, length)],
            out_specs=[
                pl.BlockSpec((1, width, block), lambda i, low, high, place: (lax.bitwise_xor(i // per, place[0]), 0, i % per)),
                pl.BlockSpec((max(8, count), block), lambda i, *_: (0, i)),
            ],
            scratch_shapes=[
                pltpu.VMEM((count, PAD, length), jnp.bfloat16),
                pltpu.VMEM((count, length, PAD), jnp.bfloat16),
                pltpu.VMEM((count, ROWS, length), jnp.bfloat16),
                pltpu.VMEM((count, length, block), jnp.float32),
                pltpu.VMEM((count, 8, block), jnp.float32),
                pltpu.VMEM((count, 8, block), jnp.float32),
                pltpu.VMEM((count, ROWS, block), jnp.float32),
            ],
        ),
        out_shape=[
            jax.ShapeDtypeStruct((length // chunk, width, chunk), jnp.bfloat16),
            jax.ShapeDtypeStruct((max(8, count), length), jnp.float32),
        ],
        compiler_params=pltpu.CompilerParams(vmem_limit_bytes=40 << 20),
        cost_estimate=pl.CostEstimate(flops=area * 800, transcendentals=area, bytes_accessed=8 * length * width),
    )(low, high, place, qkv, key_ids, query_ids)


def attend_back_kernel(
    low_ref, high_ref, place_ref, qkv_ref, out_ref, log_ref, kid_ref, qid_ref, *rest, count, block, chunks,
):
    gm_refs, grad_ref = rest[:chunks], rest[chunks]
    q_t, k_t, k_n, v_n, g_t, delta, gq, gk, gv = rest[chunks + 1 :]
    step = pl.program_id(0)
    length = qkv_ref.shape[2]
    chunk = length // chunks
    per = chunk // block
    place = place_ref[0]
    scale = HEAD_SIZE ** (-0.5)
    factor = scale * LOG2E

    @pl.when(step == 0)
    def _():
        gq[...] = jnp.zeros(gq.shape, jnp.float32)

        @pl.loop(0, length // block)
        def _(part):
            near = pl.ds(pl.multiple_of(part * block, block), block)
            at = pl.ds(pl.multiple_of(swap_chunk(part, per, place) * block, block), block)
            for h, value in enumerate(split_refs(qkv_ref[0, :, near], count)):
                q_t[h, :, at] = grow_rows(value, PAD).astype(jnp.bfloat16)
            for h, value in enumerate(split_refs(qkv_ref[1, :, near], count)):
                value = grow_rows(value, PAD)
                k_t[h, :, at] = value[:ROWS].astype(jnp.bfloat16)
                k_n[h, at, :] = value.T.astype(jnp.bfloat16)
            for h, value in enumerate(split_refs(qkv_ref[2, :, near], count)):
                v_n[h, at, :] = grow_rows(value, PAD).T.astype(jnp.bfloat16)

        for piece in range(chunks):
            at = pl.ds(pl.multiple_of(lax.bitwise_xor(piece, place) * chunk, chunk), chunk)
            grads = split_refs(gm_refs[piece][...], count)
            outs = split_refs(out_ref[piece], count)
            for h in range(count):
                g_t[h, :, at] = grow_rows(grads[h], PAD).astype(jnp.bfloat16)
                delta[h, :, at] = jnp.sum(grads[h] * outs[h], axis=0, keepdims=True)

    gk[...] = jnp.zeros(gk.shape, jnp.float32)
    gv[...] = jnp.zeros(gv.shape, jnp.float32)
    key_start = pl.multiple_of(step * block, block)
    keys = pl.ds(key_start, block)

    def one(index, _):
        query_start = pl.multiple_of(index * block, block)
        queries = pl.ds(query_start, block)
        mask = same_picture(kid_ref, qid_ref, key_start, query_start, block)
        for h in range(count):
            scores = jnp.dot(k_n[h, keys, :], q_t[h, :, queries], preferred_element_type=jnp.float32)
            probs = jnp.where(mask, jnp.exp2(scores * factor - log_ref[h : h + 1, queries]), 0.0)
            back = jnp.dot(v_n[h, keys, :], g_t[h, :, queries], preferred_element_type=jnp.float32)
            slope = (probs * (back - delta[h, :, queries])).astype(jnp.bfloat16)
            nt = (((1,), (1,)), ((), ()))
            gv[h] += lax.dot_general(
                g_t[h, :ROWS, queries], probs.astype(jnp.bfloat16), nt, preferred_element_type=jnp.float32
            )
            gk[h] += lax.dot_general(q_t[h, :ROWS, queries], slope, nt, preferred_element_type=jnp.float32)
            gq[h, :, queries] += jnp.dot(k_t[h, :, keys], slope, preferred_element_type=jnp.float32)
        return 0

    lax.fori_loop(low_ref[step], high_ref[step], one, 0)
    near = pl.ds(pl.multiple_of(swap_chunk(step, per, place) * block, block), block)
    grad_ref[1, :, near] = (jnp.concatenate([gk[h, :HEAD_SIZE] for h in range(count)], axis=0) * scale).astype(jnp.bfloat16)
    grad_ref[2, :, near] = jnp.concatenate([gv[h, :HEAD_SIZE] for h in range(count)], axis=0).astype(jnp.bfloat16)

    @pl.when(step == pl.num_programs(0) - 1)
    def _():
        @pl.loop(0, length // block)
        def _(part):
            near = pl.ds(pl.multiple_of(part * block, block), block)
            at = pl.ds(pl.multiple_of(swap_chunk(part, per, place) * block, block), block)
            grad_ref[0, :, near] = (
                jnp.concatenate([gq[h, :HEAD_SIZE, at] for h in range(count)], axis=0) * scale
            ).astype(jnp.bfloat16)


def attend_back(qkv, grad_mixed, mixed, logsum, low, high, key_ids, query_ids, place):
    _, width, length = qkv.shape
    chunk = mixed.shape[2]
    count = width // HEAD_SIZE
    block = min(256, chunk)
    whole = lambda *shape: pl.BlockSpec(shape, lambda i, *_: (0,) * len(shape))
    area = length * length * count // 2
    return pl.pallas_call(
        functools.partial(attend_back_kernel, count=count, block=block, chunks=mixed.shape[0]),
        name="attend_back",
        grid_spec=pltpu.PrefetchScalarGridSpec(
            num_scalar_prefetch=3,
            grid=(length // block,),
            in_specs=[
                whole(3, width, length),
                whole(*mixed.shape),
                whole(max(8, count), length),
                whole(length, 128),
                whole(8, length),
            ]
            + [whole(*piece.shape) for piece in grad_mixed],
            out_specs=whole(3, width, length),
            scratch_shapes=[
                pltpu.VMEM((count, PAD, length), jnp.bfloat16),
                pltpu.VMEM((count, ROWS, length), jnp.bfloat16),
                pltpu.VMEM((count, length, PAD), jnp.bfloat16),
                pltpu.VMEM((count, length, PAD), jnp.bfloat16),
                pltpu.VMEM((count, PAD, length), jnp.bfloat16),
                pltpu.VMEM((count, 1, length), jnp.float32),
                pltpu.VMEM((count, ROWS, length), jnp.float32),
                pltpu.VMEM((count, ROWS, block), jnp.float32),
                pltpu.VMEM((count, ROWS, block), jnp.float32),
            ],
        ),
        out_shape=jax.ShapeDtypeStruct((3, width, length), jnp.bfloat16),
        compiler_params=pltpu.CompilerParams(vmem_limit_bytes=60 << 20),
        cost_estimate=pl.CostEstimate(flops=area * 2000, transcendentals=area, bytes_accessed=16 * length * width),
    )(low, high, place, qkv, mixed, logsum, key_ids, query_ids, *grad_mixed)


def block_ranges(ids, block):
    ids = jnp.where(ids < 0, 1 << 20, ids).reshape(-1, block)
    first, last = ids[:, 0], ids[:, -1]
    low = jnp.sum((last[None, :] < first[:, None]).astype(jnp.int32), axis=1)
    high = jnp.sum((first[None, :] <= last[:, None]).astype(jnp.int32), axis=1)
    return low, high


def norm_parts(value_rows):
    center = value_rows - jnp.mean(value_rows, axis=-1, keepdims=True)
    inverse = lax.rsqrt(jnp.mean(center * center, axis=-1, keepdims=True) + EPS)
    return center * inverse, inverse


def norm_back(grad, normed, inverse, gain):
    scaled = grad * gain
    flat = jnp.mean(scaled, axis=-1, keepdims=True)
    along = jnp.mean(scaled * normed, axis=-1, keepdims=True)
    return inverse * (scaled - flat - normed * along)


def gelu_parts(hidden):
    first, third = math.sqrt(2 / math.pi), 0.044715 * math.sqrt(2 / math.pi)
    square = hidden * hidden
    half = 0.5 + 0.5 * jnp.tanh(hidden * (first + third * square))
    value = hidden * half
    return value, half + 2 * value * (1 - half) * (first + 3 * third * square)


def contract(left, right, left_axis, right_axis):
    return lax.dot_general(left, right, (((left_axis,), (right_axis,)), ((), ())), preferred_element_type=jnp.float32)


def per_device(
    tokens, picture_ids, attn_gain, attn_shift, query_weight, query_bias, key_weight, value_weight, value_bias,
    output_weight, output_bias, mlp_gain, mlp_shift, up_weight, up_bias, down_weight, down_bias, cotangent,
    *, seq_count, row_count,
):
    count, chunk, width = tokens.shape
    length = chunk * seq_count
    part = width // seq_count
    band_width = width // row_count
    hidden_size = up_weight.shape[1]
    slab = -(-hidden_size // (seq_count * 128)) * 128
    place = lax.axis_index("seq")
    place_array = place.reshape(1).astype(jnp.int32)
    block = min(256, chunk)
    f32, bf16 = jnp.float32, jnp.bfloat16
    rest = range(1, seq_count)

    def swap(value, hop):
        return lax.ppermute(value, "seq", [(i, i ^ hop) for i in range(seq_count)])

    def own_columns(weight):
        return lax.dynamic_slice_in_dim(weight, place * part, part, axis=1)

    def relative(stacked):
        return [lax.dynamic_index_in_dim(stacked, place ^ hop, axis=0, keepdims=False) for hop in range(seq_count)]

    whole_rows = [[tokens[row]] for row in range(count)]
    token_rows = [tokens[row] for row in range(count)]
    for row in range(count):
        if row:
            held = lax.optimization_barrier((token_rows[row], *whole_rows[row - 1][1:]))
            token_rows[row], whole_rows[row - 1][1:] = held[0], list(held[1:])
        whole_rows[row] += [swap(token_rows[row], hop) for hop in rest]

    small = [attn_gain, attn_shift, query_bias, value_bias, output_bias, mlp_gain, mlp_shift, down_bias, up_bias]
    sizes = [value.shape[0] for value in small]
    extra_rows = -(-sum(sizes) // (24 * part)) * 8

    def beside(matrix, vectors):
        lead = vectors.shape[:-1]
        vectors = jnp.pad(vectors, [(0, 0)] * len(lead) + [(0, extra_rows * 3 * part - vectors.shape[-1])])
        return jnp.concatenate([matrix, vectors.reshape(*lead, extra_rows, 3 * part)], axis=-2)

    def split(vectors):
        pieces, start = [], 0
        for size in sizes:
            pieces.append(vectors[..., start : start + size])
            start += size
        return pieces

    heads_shard = jnp.concatenate([own_columns(query_weight), own_columns(key_weight), own_columns(value_weight)], axis=1)
    heads_shard = beside(heads_shard, jnp.concatenate(small))
    gathered = lax.all_gather(heads_shard, "rows", axis=0, tiled=False)
    heads_weight = gathered[:, :band_width].reshape(width, 3 * part)
    extra = gathered[:, band_width:].reshape(row_count, extra_rows * 3 * part).astype(f32)
    gain1, shift1, query_off, value_off, output_off, gain2, shift2, down_off, up_off = [
        piece.reshape(-1) for piece in split(extra)
    ]
    up_off = relative(jnp.pad(up_off, (0, slab * seq_count - hidden_size)).reshape(seq_count, slab))
    heads_off = jnp.concatenate(
        [
            lax.dynamic_slice_in_dim(query_off, place * part, part),
            jnp.zeros((part,), f32),
            lax.dynamic_slice_in_dim(value_off, place * part, part),
        ]
    )

    def in_slabs(weight):
        return jnp.pad(weight, ((0, 0), (0, slab * seq_count - hidden_size)))

    def own_slab(weight, hop):
        return lax.dynamic_slice_in_dim(weight, (place ^ hop) * slab, slab, axis=1)

    def near_slabs(weight, hops):
        weight = in_slabs(weight)
        return lax.all_gather(jnp.concatenate([own_slab(weight, hop) for hop in hops], axis=1), "rows", axis=0, tiled=True)

    direct = list(rest)[:2]
    down_turned = down_weight.T
    down_own = near_slabs(down_turned, [0])
    output_whole = lax.all_gather(output_weight, "rows", axis=0, tiled=True)
    up_whole = near_slabs(up_weight, range(seq_count))
    late = [hop for hop in rest if hop not in direct]
    held = lax.optimization_barrier((down_own, *whole_rows[-1][1:]))
    down_own, whole_rows[-1][1:] = held[0], list(held[1:])
    downs = [down_own] + [swap(down_own, hop) for hop in direct]
    if late:
        down_turned, up_whole = lax.optimization_barrier((down_turned, up_whole))
        down_late = near_slabs(down_turned, late)
        downs += [down_late[:, i * slab : (i + 1) * slab] for i in range(len(late))]
    up_off = jnp.concatenate(up_off)
    outputs = relative(output_whole.reshape(seq_count, part, width))

    attn_inputs, packs, mixes, logs, tables, mixed_own = [], [], [], [], [], []
    for row in range(count):
        ids = picture_ids[row]
        low, high = block_ranges(ids, block)
        ids_table = (jnp.broadcast_to(ids[:, None], (length, 128)), jnp.broadcast_to(ids[None], (8, length)))
        tables.append((low, high, *ids_table))
        attn_input = jnp.concatenate(
            [(norm_parts(piece.astype(f32))[0] * gain1 + shift1).astype(bf16) for piece in whole_rows[row]], axis=0
        )
        pack = (contract(heads_weight, attn_input, 0, 1) + heads_off[:, None]).astype(bf16).reshape(3, part, length)
        mixed, logsum = attend(pack, *tables[row], place_array, chunk)
        attn_inputs.append(attn_input)
        packs.append(pack)
        mixes.append(mixed)
        logs.append(logsum)
        mixed_own.append([mixed[0]] + [swap(mixed[hop], hop) for hop in rest])

    mixed_all = jnp.concatenate(
        [jnp.concatenate([mixed_own[row][hop] for row in range(count)], axis=1) for hop in range(seq_count)], axis=0
    )
    output_near = jnp.concatenate(outputs, axis=0)
    tokens_own = tokens.reshape(count * chunk, width).astype(f32)
    resid = tokens_own + (contract(mixed_all, output_near, 0, 0) + output_off)
    normed2, inverse2 = norm_parts(resid)
    mlp_input = (normed2 * gain2 + shift2).astype(bf16)
    total = None
    hidden = contract(mlp_input, up_whole, 1, 0) + up_off
    gelu_out, slope = gelu_parts(hidden)
    gelu_out, slope = gelu_out.astype(bf16), slope.astype(bf16)

    def slab_of(value, hop):
        return value[:, hop * slab : (hop + 1) * slab]

    def all_pieces(share):
        stacked = jnp.stack([share] + [swap(share, hop) for hop in rest])
        return relative(stacked)

    def exchange_sum(pieces):
        total = pieces[0].astype(f32)
        for hop in rest:
            total = total + swap(pieces[hop], hop).astype(f32)
        return total

    cot = cotangent.reshape(count * chunk, width)
    grad_down = with_layout_constraint(contract(cot, gelu_out, 0, 0).astype(bf16), Layout(major_to_minor=(0, 1)))
    cot, grad_down = lax.optimization_barrier((cot, grad_down))
    down_raw = lax.psum_scatter(grad_down, "rows", scatter_dimension=0, tiled=True)
    grad_hidden = jnp.concatenate(
        [(contract(cot, downs[hop], 1, 0) * slab_of(slope, hop).astype(f32)).astype(bf16) for hop in range(seq_count)], axis=1
    )
    grad_mlp_input = contract(grad_hidden, up_whole, 1, 1)
    grad_up = contract(mlp_input, grad_hidden, 0, 0).astype(bf16)
    grad_resid = cot.astype(f32) + norm_back(grad_mlp_input, normed2, inverse2, gain2)
    grad_attn = grad_resid.astype(bf16)

    grad_output = contract(mixed_all, grad_attn, 1, 0)
    grad_output = relative(grad_output.astype(bf16).reshape(seq_count, part, width))
    grad_output = jnp.concatenate(grad_output, axis=0)
    mixed_grads = []
    for row in range(count):
        pieces = []
        for hop in range(seq_count):
            piece = contract(outputs[hop], grad_attn[row * chunk : (row + 1) * chunk], 1, 1).astype(bf16)
            pieces.append(swap(piece, hop) if hop else piece)
        mixed_grads.append(pieces)
    held = lax.optimization_barrier((packs[0], down_raw, grad_up, grad_output, *mixed_grads[0]))
    packs[0], down_raw, grad_up, grad_output = held[:4]
    mixed_grads[0] = list(held[4:])
    up_raw = lax.psum_scatter(grad_up, "rows", scatter_dimension=0, tiled=True)
    down_share = exchange_sum([slab_of(down_raw, hop) for hop in range(seq_count)]).astype(bf16)
    down_pieces = all_pieces(down_share)
    heads_grad, query_grad, value_grad, gain_grad, shift_grad, grad_in = None, 0.0, 0.0, 0.0, 0.0, []
    after = None
    for row in range(count):
        grad_mixed = mixed_grads[row]
        pack = packs[row]
        if after is not None:
            pack, grad_in[-1] = lax.optimization_barrier((pack, grad_in[-1]))
        grad_pack = attend_back(pack, grad_mixed, mixes[row], logs[row], *tables[row], place_array)
        if row == count - 1:
            grad_pack, up_raw, grad_output = lax.optimization_barrier((grad_pack, up_raw, grad_output))
            output_share = lax.psum_scatter(grad_output, "rows", scatter_dimension=0, tiled=True)
        query_grad = query_grad + jnp.sum(grad_pack[0].astype(f32), axis=1)
        value_grad = value_grad + jnp.sum(grad_pack[2].astype(f32), axis=1)
        grad_pack = grad_pack.reshape(3 * part, length)
        partial = []
        for hop in range(seq_count):
            piece = contract(grad_pack[:, hop * chunk : (hop + 1) * chunk], heads_weight, 0, 1)
            gain_grad = gain_grad + jnp.sum(piece * norm_parts(whole_rows[row][hop].astype(f32))[0], axis=0)
            shift_grad = shift_grad + jnp.sum(piece, axis=0)
            partial.append(piece.astype(bf16))
        grad_in.append(partial)
        after = partial
        term = contract(attn_inputs[row], grad_pack, 0, 1)
        heads_grad = term if heads_grad is None else heads_grad + term

    def placed(value):
        return lax.dynamic_update_slice_in_dim(jnp.zeros((width,), f32), value, place * part, axis=0)

    up_grads = jnp.stack(relative(jnp.sum(grad_hidden.astype(f32), axis=0).reshape(seq_count, slab)))
    small_grads = [
        gain_grad,
        shift_grad,
        placed(query_grad),
        placed(value_grad),
        jnp.sum(grad_attn.astype(f32), axis=0),
        jnp.sum(grad_mlp_input * normed2, axis=0),
        jnp.sum(grad_mlp_input, axis=0),
        jnp.sum(cot.astype(f32), axis=0),
        up_grads.reshape(slab * seq_count)[:hidden_size],
    ]
    together = jnp.concatenate([value.reshape(row_count, -1) for value in small_grads], axis=1).astype(bf16)
    heads_grad = beside(heads_grad.astype(bf16).reshape(row_count, band_width, 3 * part), together)
    held = lax.optimization_barrier((heads_grad, output_share, *[pieces[0] for pieces in grad_in]))
    heads_grad, output_share = held[:2]
    for row in range(count):
        grad_in[row][0] = held[2 + row]
    gelu_late, output_share, up_raw, heads_grad = lax.optimization_barrier((gelu_out, output_share, up_raw, heads_grad))
    total = resid
    for hop in range(seq_count):
        total = total + contract(slab_of(gelu_late, hop), downs[hop], 1, 1)
    activations = total + down_off
    up_share = exchange_sum([slab_of(up_raw, hop) for hop in range(seq_count)]).astype(bf16)

    heads_share = lax.psum_scatter(heads_grad, "rows", scatter_dimension=0, tiled=False)
    normed1, inverse1 = norm_parts(tokens_own)
    sums = []
    for row in range(count):
        sums.append(exchange_sum(grad_in[row]))
    grad_attn_input = jnp.concatenate(sums, axis=0)
    token_grad = grad_resid + norm_back(grad_attn_input, normed1, inverse1, gain1)

    def seq_sum(share):
        total = share.astype(f32)
        for hop in rest:
            total = total + swap(share, hop).astype(f32)
        return total

    heads_all = [piece.astype(f32) for piece in all_pieces(heads_share)]
    small_sum = sum(piece[band_width:] for piece in heads_all).reshape(extra_rows * 3 * part)
    vectors = split(small_sum)

    def take(which):
        return jnp.concatenate([piece[:band_width, which * part : (which + 1) * part] for piece in heads_all], axis=1)

    def slabs(pieces):
        return jnp.concatenate([piece.astype(f32) for piece in pieces], axis=1)[:, :hidden_size]

    return (
        activations.reshape(count, chunk, width),
        token_grad.reshape(count, chunk, width),
        vectors[0],
        vectors[1],
        take(0),
        vectors[2],
        take(1),
        take(2),
        vectors[3],
        seq_sum(output_share),
        vectors[4],
        vectors[5],
        vectors[6],
        slabs(all_pieces(up_share)),
        vectors[8],
        slabs(down_pieces).T,
        vectors[7],
    )


def solution(mesh):
    matrix, vector, batch = P("rows", None), P("rows"), P("rows", "seq", None)
    columns = P(None, "rows")

    def body(*arguments):
        return per_device(*arguments, seq_count=mesh.shape["seq"], row_count=mesh.shape["rows"])

    return jax.shard_map(
        body,
        mesh=mesh,
        in_specs=(
            batch, matrix, vector, vector, matrix, vector, matrix, matrix, vector, matrix, vector, vector, vector, matrix,
            vector, columns, vector, batch,
        ),
        out_specs=(
            batch, batch, vector, vector, matrix, vector, matrix, matrix, vector, matrix, vector, vector, vector, matrix,
            vector, columns, vector,
        ),
        check_vma=False,
    )
```

```python
import functools
import math

import jax
import jax.numpy as jnp
from jax import lax
from jax.experimental import pallas as pl
from jax.experimental.layout import Layout, with_layout_constraint
from jax.experimental.pallas import tpu as pltpu
from jax.sharding import PartitionSpec as P


HEAD_SIZE = 72
EPS = 1e-06
NEGATIVE = -1e30
LOG2E = 1.4426950408889634
PAD = 128
ROWS = 80


def split_refs(source, count):
    wide = source.astype(jnp.float32)
    return [wide[HEAD_SIZE * h : HEAD_SIZE * (h + 1)] for h in range(count)]


def grow_rows(value, rows):
    return jnp.concatenate([value, jnp.zeros((rows - value.shape[0], value.shape[1]), value.dtype)], axis=0)


def swap_chunk(part, per, place):
    return lax.bitwise_xor(part // per, place) * per + part % per


def same_picture(kid_ref, qid_ref, key_start, query_start, block):
    key_ids = kid_ref[pl.ds(key_start, block), :]
    key_ids = jnp.concatenate([key_ids] * (block // 128), axis=1)
    return key_ids == qid_ref[0:1, pl.ds(query_start, block)]


def attend_kernel(low_ref, high_ref, place_ref, qkv_ref, kid_ref, qid_ref, out_ref, log_ref, q_t, k_n, v_t, kept, top, total, acc, *, count, block, chunk):
    step = pl.program_id(0)
    length = qkv_ref.shape[2]
    per = chunk // block
    factor = HEAD_SIZE ** (-0.5) * LOG2E

    @pl.when(step == 0)
    def _():
        @pl.loop(0, length // block)
        def _(part):
            near = pl.ds(pl.multiple_of(part * block, block), block)
            at = pl.ds(pl.multiple_of(swap_chunk(part, per, place_ref[0]) * block, block), block)
            for h, value in enumerate(split_refs(qkv_ref[0, :, near], count)):
                q_t[h, :, at] = grow_rows(value, PAD).astype(jnp.bfloat16)
            for h, value in enumerate(split_refs(qkv_ref[1, :, near], count)):
                k_n[h, at, :] = grow_rows(value, PAD).T.astype(jnp.bfloat16)
            for h, value in enumerate(split_refs(qkv_ref[2, :, near], count)):
                v_t[h, :, at] = grow_rows(value, ROWS).astype(jnp.bfloat16)

    top[...] = jnp.full(top.shape, NEGATIVE, jnp.float32)
    total[...] = jnp.zeros(total.shape, jnp.float32)
    acc[...] = jnp.zeros(acc.shape, jnp.float32)
    query_start = pl.multiple_of(step * block, block)
    queries = pl.ds(query_start, block)

    def first(index, _):
        key_start = pl.multiple_of(index * block, block)
        mask = same_picture(kid_ref, qid_ref, key_start, query_start, block)
        for h in range(count):
            scores = jnp.dot(
                k_n[h, pl.ds(key_start, block), :], q_t[h, :, queries], preferred_element_type=jnp.float32
            )
            scores = jnp.where(mask, scores * factor, NEGATIVE)
            kept[h, pl.ds(key_start, block), :] = scores
            top[h] = jnp.maximum(top[h], jnp.max(scores.reshape(block // 8, 8, block), axis=0))
        return 0

    lax.fori_loop(low_ref[step], high_ref[step], first, 0)
    highest = [jnp.max(top[h], axis=0, keepdims=True) for h in range(count)]

    def second(index, _):
        keys = pl.ds(pl.multiple_of(index * block, block), block)
        for h in range(count):
            probs = jnp.exp2(kept[h, keys, :] - highest[h])
            total[h] += jnp.sum(probs.reshape(block // 8, 8, block), axis=0)
            acc[h] += jnp.dot(v_t[h, :, keys], probs.astype(jnp.bfloat16), preferred_element_type=jnp.float32)
        return 0

    lax.fori_loop(low_ref[step], high_ref[step], second, 0)
    sums = [jnp.sum(total[h], axis=0, keepdims=True) for h in range(count)]
    for h in range(count):
        log_ref[h : h + 1, :] = highest[h] + jnp.log2(sums[h])
    out_ref[0] = jnp.concatenate([acc[h, :HEAD_SIZE] / sums[h] for h in range(count)], axis=0).astype(jnp.bfloat16)


def attend(qkv, low, high, key_ids, query_ids, place, chunk):
    _, width, length = qkv.shape
    count = width // HEAD_SIZE
    block = min(256, chunk)
    per = chunk // block
    whole = lambda *shape: pl.BlockSpec(shape, lambda i, *_: (0,) * len(shape))
    area = length * length * count // 2
    return pl.pallas_call(
        functools.partial(attend_kernel, count=count, block=block, chunk=chunk),
        name="attend",
        grid_spec=pltpu.PrefetchScalarGridSpec(
            num_scalar_prefetch=3,
            grid=(length // block,),
            in_specs=[whole(3, width, length), whole(length, 128), whole(8, length)],
            out_specs=[
                pl.BlockSpec((1, width, block), lambda i, low, high, place: (lax.bitwise_xor(i // per, place[0]), 0, i % per)),
                pl.BlockSpec((max(8, count), block), lambda i, *_: (0, i)),
            ],
            scratch_shapes=[
                pltpu.VMEM((count, PAD, length), jnp.bfloat16),
                pltpu.VMEM((count, length, PAD), jnp.bfloat16),
                pltpu.VMEM((count, ROWS, length), jnp.bfloat16),
                pltpu.VMEM((count, length, block), jnp.float32),
                pltpu.VMEM((count, 8, block), jnp.float32),
                pltpu.VMEM((count, 8, block), jnp.float32),
                pltpu.VMEM((count, ROWS, block), jnp.float32),
            ],
        ),
        out_shape=[
            jax.ShapeDtypeStruct((length // chunk, width, chunk), jnp.bfloat16),
            jax.ShapeDtypeStruct((max(8, count), length), jnp.float32),
        ],
        compiler_params=pltpu.CompilerParams(vmem_limit_bytes=40 << 20),
        cost_estimate=pl.CostEstimate(flops=area * 800, transcendentals=area, bytes_accessed=8 * length * width),
    )(low, high, place, qkv, key_ids, query_ids)


def attend_back_kernel(
    low_ref, high_ref, place_ref, qkv_ref, out_ref, log_ref, kid_ref, qid_ref, *rest, count, block, chunks,
):
    gm_refs, grad_ref = rest[:chunks], rest[chunks]
    q_t, k_t, k_n, v_n, g_t, delta, gq, gk, gv = rest[chunks + 1 :]
    step = pl.program_id(0)
    length = qkv_ref.shape[2]
    chunk = length // chunks
    per = chunk // block
    place = place_ref[0]
    scale = HEAD_SIZE ** (-0.5)
    factor = scale * LOG2E

    @pl.when(step == 0)
    def _():
        gq[...] = jnp.zeros(gq.shape, jnp.float32)

        @pl.loop(0, length // block)
        def _(part):
            near = pl.ds(pl.multiple_of(part * block, block), block)
            at = pl.ds(pl.multiple_of(swap_chunk(part, per, place) * block, block), block)
            for h, value in enumerate(split_refs(qkv_ref[0, :, near], count)):
                q_t[h, :, at] = grow_rows(value, PAD).astype(jnp.bfloat16)
            for h, value in enumerate(split_refs(qkv_ref[1, :, near], count)):
                value = grow_rows(value, PAD)
                k_t[h, :, at] = value[:ROWS].astype(jnp.bfloat16)
                k_n[h, at, :] = value.T.astype(jnp.bfloat16)
            for h, value in enumerate(split_refs(qkv_ref[2, :, near], count)):
                v_n[h, at, :] = grow_rows(value, PAD).T.astype(jnp.bfloat16)

        for piece in range(chunks):
            at = pl.ds(pl.multiple_of(lax.bitwise_xor(piece, place) * chunk, chunk), chunk)
            grads = split_refs(gm_refs[piece][...], count)
            outs = split_refs(out_ref[piece], count)
            for h in range(count):
                g_t[h, :, at] = grow_rows(grads[h], PAD).astype(jnp.bfloat16)
                delta[h, :, at] = jnp.sum(grads[h] * outs[h], axis=0, keepdims=True)

    gk[...] = jnp.zeros(gk.shape, jnp.float32)
    gv[...] = jnp.zeros(gv.shape, jnp.float32)
    key_start = pl.multiple_of(step * block, block)
    keys = pl.ds(key_start, block)

    def one(index, _):
        query_start = pl.multiple_of(index * block, block)
        queries = pl.ds(query_start, block)
        mask = same_picture(kid_ref, qid_ref, key_start, query_start, block)
        for h in range(count):
            scores = jnp.dot(k_n[h, keys, :], q_t[h, :, queries], preferred_element_type=jnp.float32)
            probs = jnp.where(mask, jnp.exp2(scores * factor - log_ref[h : h + 1, queries]), 0.0)
            back = jnp.dot(v_n[h, keys, :], g_t[h, :, queries], preferred_element_type=jnp.float32)
            slope = (probs * (back - delta[h, :, queries])).astype(jnp.bfloat16)
            nt = (((1,), (1,)), ((), ()))
            gv[h] += lax.dot_general(
                g_t[h, :ROWS, queries], probs.astype(jnp.bfloat16), nt, preferred_element_type=jnp.float32
            )
            gk[h] += lax.dot_general(q_t[h, :ROWS, queries], slope, nt, preferred_element_type=jnp.float32)
            gq[h, :, queries] += jnp.dot(k_t[h, :, keys], slope, preferred_element_type=jnp.float32)
        return 0

    lax.fori_loop(low_ref[step], high_ref[step], one, 0)
    near = pl.ds(pl.multiple_of(swap_chunk(step, per, place) * block, block), block)
    grad_ref[1, :, near] = (jnp.concatenate([gk[h, :HEAD_SIZE] for h in range(count)], axis=0) * scale).astype(jnp.bfloat16)
    grad_ref[2, :, near] = jnp.concatenate([gv[h, :HEAD_SIZE] for h in range(count)], axis=0).astype(jnp.bfloat16)

    @pl.when(step == pl.num_programs(0) - 1)
    def _():
        @pl.loop(0, length // block)
        def _(part):
            near = pl.ds(pl.multiple_of(part * block, block), block)
            at = pl.ds(pl.multiple_of(swap_chunk(part, per, place) * block, block), block)
            grad_ref[0, :, near] = (
                jnp.concatenate([gq[h, :HEAD_SIZE, at] for h in range(count)], axis=0) * scale
            ).astype(jnp.bfloat16)


def attend_back(qkv, grad_mixed, mixed, logsum, low, high, key_ids, query_ids, place):
    _, width, length = qkv.shape
    chunk = mixed.shape[2]
    count = width // HEAD_SIZE
    block = min(256, chunk)
    whole = lambda *shape: pl.BlockSpec(shape, lambda i, *_: (0,) * len(shape))
    area = length * length * count // 2
    return pl.pallas_call(
        functools.partial(attend_back_kernel, count=count, block=block, chunks=mixed.shape[0]),
        name="attend_back",
        grid_spec=pltpu.PrefetchScalarGridSpec(
            num_scalar_prefetch=3,
            grid=(length // block,),
            in_specs=[
                whole(3, width, length),
                whole(*mixed.shape),
                whole(max(8, count), length),
                whole(length, 128),
                whole(8, length),
            ]
            + [whole(*piece.shape) for piece in grad_mixed],
            out_specs=whole(3, width, length),
            scratch_shapes=[
                pltpu.VMEM((count, PAD, length), jnp.bfloat16),
                pltpu.VMEM((count, ROWS, length), jnp.bfloat16),
                pltpu.VMEM((count, length, PAD), jnp.bfloat16),
                pltpu.VMEM((count, length, PAD), jnp.bfloat16),
                pltpu.VMEM((count, PAD, length), jnp.bfloat16),
                pltpu.VMEM((count, 1, length), jnp.float32),
                pltpu.VMEM((count, ROWS, length), jnp.float32),
                pltpu.VMEM((count, ROWS, block), jnp.float32),
                pltpu.VMEM((count, ROWS, block), jnp.float32),
            ],
        ),
        out_shape=jax.ShapeDtypeStruct((3, width, length), jnp.bfloat16),
        compiler_params=pltpu.CompilerParams(vmem_limit_bytes=60 << 20),
        cost_estimate=pl.CostEstimate(flops=area * 2000, transcendentals=area, bytes_accessed=16 * length * width),
    )(low, high, place, qkv, mixed, logsum, key_ids, query_ids, *grad_mixed)


def block_ranges(ids, block):
    ids = jnp.where(ids < 0, 1 << 20, ids).reshape(-1, block)
    first, last = ids[:, 0], ids[:, -1]
    low = jnp.sum((last[None, :] < first[:, None]).astype(jnp.int32), axis=1)
    high = jnp.sum((first[None, :] <= last[:, None]).astype(jnp.int32), axis=1)
    return low, high


def norm_parts(value_rows):
    center = value_rows - jnp.mean(value_rows, axis=-1, keepdims=True)
    inverse = lax.rsqrt(jnp.mean(center * center, axis=-1, keepdims=True) + EPS)
    return center * inverse, inverse


def norm_back(grad, normed, inverse, gain):
    scaled = grad * gain
    flat = jnp.mean(scaled, axis=-1, keepdims=True)
    along = jnp.mean(scaled * normed, axis=-1, keepdims=True)
    return inverse * (scaled - flat - normed * along)


def gelu_parts(hidden):
    first, third = math.sqrt(2 / math.pi), 0.044715 * math.sqrt(2 / math.pi)
    square = hidden * hidden
    half = 0.5 + 0.5 * jnp.tanh(hidden * (first + third * square))
    value = hidden * half
    return value, half + 2 * value * (1 - half) * (first + 3 * third * square)


def contract(left, right, left_axis, right_axis):
    return lax.dot_general(left, right, (((left_axis,), (right_axis,)), ((), ())), preferred_element_type=jnp.float32)


def per_device(
    tokens, picture_ids, attn_gain, attn_shift, query_weight, query_bias, key_weight, value_weight, value_bias,
    output_weight, output_bias, mlp_gain, mlp_shift, up_weight, up_bias, down_weight, down_bias, cotangent,
    *, seq_count, row_count,
):
    count, chunk, width = tokens.shape
    length = chunk * seq_count
    part = width // seq_count
    band_width = width // row_count
    hidden_size = up_weight.shape[1]
    slab = -(-hidden_size // (seq_count * 128)) * 128
    place = lax.axis_index("seq")
    place_array = place.reshape(1).astype(jnp.int32)
    block = min(256, chunk)
    f32, bf16 = jnp.float32, jnp.bfloat16
    rest = range(1, seq_count)

    def swap(value, hop):
        return lax.ppermute(value, "seq", [(i, i ^ hop) for i in range(seq_count)])

    def own_columns(weight):
        return lax.dynamic_slice_in_dim(weight, place * part, part, axis=1)

    def relative(stacked):
        return [lax.dynamic_index_in_dim(stacked, place ^ hop, axis=0, keepdims=False) for hop in range(seq_count)]

    whole_rows = [[tokens[row]] for row in range(count)]
    token_rows = [tokens[row] for row in range(count)]
    for row in range(count):
        if row:
            held = lax.optimization_barrier((token_rows[row], *whole_rows[row - 1][1:]))
            token_rows[row], whole_rows[row - 1][1:] = held[0], list(held[1:])
        whole_rows[row] += [swap(token_rows[row], hop) for hop in rest]

    small = [attn_gain, attn_shift, query_bias, value_bias, output_bias, mlp_gain, mlp_shift, down_bias, up_bias]
    sizes = [value.shape[0] for value in small]
    extra_rows = -(-sum(sizes) // (24 * part)) * 8

    def beside(matrix, vectors):
        lead = vectors.shape[:-1]
        vectors = jnp.pad(vectors, [(0, 0)] * len(lead) + [(0, extra_rows * 3 * part - vectors.shape[-1])])
        return jnp.concatenate([matrix, vectors.reshape(*lead, extra_rows, 3 * part)], axis=-2)

    def split(vectors):
        pieces, start = [], 0
        for size in sizes:
            pieces.append(vectors[..., start : start + size])
            start += size
        return pieces

    heads_shard = jnp.concatenate([own_columns(query_weight), own_columns(key_weight), own_columns(value_weight)], axis=1)
    heads_shard = beside(heads_shard, jnp.concatenate(small))
    gathered = lax.all_gather(heads_shard, "rows", axis=0, tiled=False)
    heads_weight = gathered[:, :band_width].reshape(width, 3 * part)
    extra = gathered[:, band_width:].reshape(row_count, extra_rows * 3 * part).astype(f32)
    gain1, shift1, query_off, value_off, output_off, gain2, shift2, down_off, up_off = [
        piece.reshape(-1) for piece in split(extra)
    ]
    up_off = relative(jnp.pad(up_off, (0, slab * seq_count - hidden_size)).reshape(seq_count, slab))
    heads_off = jnp.concatenate(
        [
            lax.dynamic_slice_in_dim(query_off, place * part, part),
            jnp.zeros((part,), f32),
            lax.dynamic_slice_in_dim(value_off, place * part, part),
        ]
    )

    def in_slabs(weight):
        return jnp.pad(weight, ((0, 0), (0, slab * seq_count - hidden_size)))

    def own_slab(weight, hop):
        return lax.dynamic_slice_in_dim(weight, (place ^ hop) * slab, slab, axis=1)

    def near_slabs(weight, hops):
        weight = in_slabs(weight)
        return lax.all_gather(jnp.concatenate([own_slab(weight, hop) for hop in hops], axis=1), "rows", axis=0, tiled=True)

    direct = list(rest)[:2]
    down_turned = down_weight.T
    down_own = near_slabs(down_turned, [0])
    output_whole = lax.all_gather(output_weight, "rows", axis=0, tiled=True)
    halves = [range(seq_count // 2), range(seq_count // 2, seq_count)]
    ups = [near_slabs(up_weight, hops) for hops in halves]
    late = [hop for hop in rest if hop not in direct]
    down_turned, ups[1] = lax.optimization_barrier((down_turned, ups[1]))
    down_late = near_slabs(down_turned, late) if late else None
    up_off = jnp.concatenate(up_off)
    outputs = relative(output_whole.reshape(seq_count, part, width))

    normed_rows, packs, mixes, logs, tables, mixed_own = [], [], [], [], [], []
    for row in range(count):
        ids = picture_ids[row]
        low, high = block_ranges(ids, block)
        ids_table = (jnp.broadcast_to(ids[:, None], (length, 128)), jnp.broadcast_to(ids[None], (8, length)))
        tables.append((low, high, *ids_table))
        normed_pieces = [norm_parts(piece.astype(f32))[0] for piece in whole_rows[row]]
        attn_input = jnp.concatenate([(piece * gain1 + shift1).astype(bf16) for piece in normed_pieces], axis=0)
        normed_rows.append(jnp.concatenate([piece.astype(bf16) for piece in normed_pieces], axis=0))
        pack = (contract(heads_weight, attn_input, 0, 1) + heads_off[:, None]).astype(bf16).reshape(3, part, length)
        mixed, logsum = attend(pack, *tables[row], place_array, chunk)
        packs.append(pack)
        mixes.append(mixed)
        logs.append(logsum)
        mixed_own.append([mixed[0]] + [swap(mixed[hop], hop) for hop in rest])

    held = lax.optimization_barrier((down_own, *mixed_own[-1][1:]))
    down_own, mixed_own[-1][1:] = held[0], list(held[1:])
    downs = [down_own] + [swap(down_own, hop) for hop in direct]
    downs += [down_late[:, i * slab : (i + 1) * slab] for i in range(len(late))]

    mixed_all = jnp.concatenate(
        [jnp.concatenate([mixed_own[row][hop] for row in range(count)], axis=1) for hop in range(seq_count)], axis=0
    )
    output_near = jnp.concatenate(outputs, axis=0)
    tokens_own = tokens.reshape(count * chunk, width).astype(f32)
    resid = tokens_own + (contract(mixed_all, output_near, 0, 0) + output_off)
    normed2, inverse2 = norm_parts(resid)
    mlp_input = (normed2 * gain2 + shift2).astype(bf16)
    parts = []
    for hops, weight in zip(halves, ups):
        offset = up_off[hops[0] * slab : (hops[-1] + 1) * slab]
        parts.append([v.astype(bf16) for v in gelu_parts(contract(mlp_input, weight, 1, 0) + offset)])
    gelu_out = jnp.concatenate([pair[0] for pair in parts], axis=1)
    slope = jnp.concatenate([pair[1] for pair in parts], axis=1)

    def slab_of(value, hop):
        return value[:, hop * slab : (hop + 1) * slab]

    def all_pieces(share):
        stacked = jnp.stack([share] + [swap(share, hop) for hop in rest])
        return relative(stacked)

    def exchange_sum(pieces):
        total = pieces[0].astype(f32)
        for hop in rest:
            total = total + swap(pieces[hop], hop).astype(f32)
        return total

    cot = cotangent.reshape(count * chunk, width)
    grad_down = with_layout_constraint(contract(cot, gelu_out, 0, 0).astype(bf16), Layout(major_to_minor=(0, 1)))
    cot, grad_down = lax.optimization_barrier((cot, grad_down))
    down_raw = lax.psum_scatter(grad_down, "rows", scatter_dimension=0, tiled=True)
    grad_pieces = [(contract(cot, downs[hop], 1, 0) * slab_of(slope, hop).astype(f32)).astype(bf16) for hop in range(seq_count)]
    up_grads = jnp.stack(relative(jnp.stack([jnp.sum(piece.astype(f32), axis=0) for piece in grad_pieces])))
    grad_hidden = jnp.concatenate(grad_pieces, axis=1)
    grad_mlp_input = None
    for hops, weight in zip(halves, ups):
        term = contract(grad_hidden[:, hops[0] * slab : (hops[-1] + 1) * slab], weight, 1, 1)
        grad_mlp_input = term if grad_mlp_input is None else grad_mlp_input + term
    grad_up = contract(mlp_input, grad_hidden, 0, 0).astype(bf16)
    grad_resid = cot.astype(f32) + norm_back(grad_mlp_input, normed2, inverse2, gain2)
    grad_attn = grad_resid.astype(bf16)

    grad_output = contract(mixed_all, grad_attn, 1, 0)
    grad_output = relative(grad_output.astype(bf16).reshape(seq_count, part, width))
    grad_output = jnp.concatenate(grad_output, axis=0)
    mixed_grads = []
    for row in range(count):
        pieces = []
        for hop in range(seq_count):
            piece = contract(outputs[hop], grad_attn[row * chunk : (row + 1) * chunk], 1, 1).astype(bf16)
            pieces.append(swap(piece, hop) if hop else piece)
        mixed_grads.append(pieces)
    held = lax.optimization_barrier((packs[0], down_raw, grad_up, grad_output, *mixed_grads[0]))
    packs[0], down_raw, grad_up, grad_output = held[:4]
    mixed_grads[0] = list(held[4:])
    up_raw = lax.psum_scatter(grad_up, "rows", scatter_dimension=0, tiled=True)
    down_share = exchange_sum([slab_of(down_raw, hop) for hop in range(seq_count)]).astype(bf16)
    down_pieces = all_pieces(down_share)
    normed_grad, sum_grad, grad_in = None, 0.0, []
    early_grads = [
        jnp.sum(grad_attn.astype(f32), axis=0),
        jnp.sum(grad_mlp_input * normed2, axis=0),
        jnp.sum(grad_mlp_input, axis=0),
        jnp.sum(cot.astype(f32), axis=0),
        up_grads.reshape(slab * seq_count)[:hidden_size],
    ]
    early_grads = jnp.concatenate([value.reshape(row_count, -1) for value in early_grads], axis=1)
    after = None
    for row in range(count):
        grad_mixed = mixed_grads[row]
        pack = packs[row]
        if after is not None:
            pack, grad_in[-1], early_grads = lax.optimization_barrier((pack, grad_in[-1], early_grads))
        grad_pack = attend_back(pack, grad_mixed, mixes[row], logs[row], *tables[row], place_array)
        if row == count - 1:
            grad_pack, up_raw, grad_output = lax.optimization_barrier((grad_pack, up_raw, grad_output))
            output_share = lax.psum_scatter(grad_output, "rows", scatter_dimension=0, tiled=True)
        grad_pack = grad_pack.reshape(3 * part, length)
        sum_grad = sum_grad + jnp.sum(grad_pack.astype(f32), axis=1)
        partial = []
        for hop in range(seq_count):
            piece = contract(grad_pack[:, hop * chunk : (hop + 1) * chunk], heads_weight, 0, 1)
            partial.append(piece.astype(bf16))
        grad_in.append(partial)
        after = partial
        term = with_layout_constraint(contract(normed_rows[row], grad_pack, 0, 1), Layout(major_to_minor=(0, 1)))
        normed_grad = term if normed_grad is None else normed_grad + term

    def placed(value):
        return lax.dynamic_update_slice_in_dim(jnp.zeros((width,), f32), value, place * part, axis=0)

    wide_weight = heads_weight.astype(f32)
    heads_grad = gain1[:, None] * normed_grad + shift1[:, None] * sum_grad
    late_grads = [
        jnp.sum(wide_weight * normed_grad, axis=1),
        jnp.sum(wide_weight * sum_grad, axis=1),
        placed(sum_grad[:part]),
        placed(sum_grad[2 * part :]),
    ]
    together = jnp.concatenate([value.reshape(row_count, -1) for value in late_grads] + [early_grads], axis=1).astype(bf16)
    heads_grad = beside(heads_grad.astype(bf16).reshape(row_count, band_width, 3 * part), together)
    held = lax.optimization_barrier((heads_grad, output_share, *[pieces[0] for pieces in grad_in]))
    heads_grad, output_share = held[:2]
    for row in range(count):
        grad_in[row][0] = held[2 + row]
    gelu_late, output_share, up_raw, heads_grad = lax.optimization_barrier((gelu_out, output_share, up_raw, heads_grad))
    total = resid
    for hop in range(seq_count):
        total = total + contract(slab_of(gelu_late, hop), downs[hop], 1, 1)
    activations = total + down_off
    up_share = exchange_sum([slab_of(up_raw, hop) for hop in range(seq_count)]).astype(bf16)

    heads_share = lax.psum_scatter(heads_grad, "rows", scatter_dimension=0, tiled=False)
    normed1, inverse1 = norm_parts(tokens_own)
    sums = []
    for row in range(count):
        sums.append(exchange_sum(grad_in[row]))
    grad_attn_input = jnp.concatenate(sums, axis=0)
    token_grad = grad_resid + norm_back(grad_attn_input, normed1, inverse1, gain1)

    def seq_sum(share):
        total = share.astype(f32)
        for hop in rest:
            total = total + swap(share, hop).astype(f32)
        return total

    heads_all = [piece.astype(f32) for piece in all_pieces(heads_share)]
    small_sum = sum(piece[band_width:] for piece in heads_all).reshape(extra_rows * 3 * part)
    vectors = split(small_sum)

    def take(which):
        return jnp.concatenate([piece[:band_width, which * part : (which + 1) * part] for piece in heads_all], axis=1)

    def slabs(pieces):
        return jnp.concatenate([piece.astype(f32) for piece in pieces], axis=1)[:, :hidden_size]

    return (
        activations.reshape(count, chunk, width),
        token_grad.reshape(count, chunk, width),
        vectors[0],
        vectors[1],
        take(0),
        vectors[2],
        take(1),
        take(2),
        vectors[3],
        seq_sum(output_share),
        vectors[4],
        vectors[5],
        vectors[6],
        slabs(all_pieces(up_share)),
        vectors[8],
        slabs(down_pieces).T,
        vectors[7],
    )


def solution(mesh):
    matrix, vector, batch = P("rows", None), P("rows"), P("rows", "seq", None)
    columns = P(None, "rows")

    def body(*arguments):
        return per_device(*arguments, seq_count=mesh.shape["seq"], row_count=mesh.shape["rows"])

    return jax.shard_map(
        body,
        mesh=mesh,
        in_specs=(
            batch, matrix, vector, vector, matrix, vector, matrix, matrix, vector, matrix, vector, vector, vector, matrix,
            vector, columns, vector, batch,
        ),
        out_specs=(
            batch, batch, vector, vector, matrix, vector, matrix, matrix, vector, matrix, vector, vector, vector, matrix,
            vector, columns, vector,
        ),
        check_vma=False,
    )
```

```python
import functools
import math

import jax
import jax.numpy as jnp
from jax import lax
from jax.experimental import pallas as pl
from jax.experimental.layout import Layout, with_layout_constraint
from jax.experimental.pallas import tpu as pltpu
from jax.sharding import PartitionSpec as P


HEAD_SIZE = 72
EPS = 1e-06
NEGATIVE = -1e30
LOG2E = 1.4426950408889634
PAD = 128
ROWS = 80


def split_refs(source, count):
    wide = source.astype(jnp.float32)
    return [wide[HEAD_SIZE * h : HEAD_SIZE * (h + 1)] for h in range(count)]


def grow_rows(value, rows):
    return jnp.concatenate([value, jnp.zeros((rows - value.shape[0], value.shape[1]), value.dtype)], axis=0)


def swap_chunk(part, per, place):
    return lax.bitwise_xor(part // per, place) * per + part % per


def same_picture(kid_ref, qid_ref, key_start, query_start, block):
    key_ids = kid_ref[pl.ds(key_start, block), :]
    key_ids = jnp.concatenate([key_ids] * (block // 128), axis=1)
    return key_ids == qid_ref[0:1, pl.ds(query_start, block)]


def attend_kernel(low_ref, high_ref, place_ref, qkv_ref, kid_ref, qid_ref, out_ref, log_ref, q_t, k_n, v_t, kept, top, total, acc, *, count, block, chunk):
    step = pl.program_id(0)
    length = qkv_ref.shape[2]
    per = chunk // block
    factor = HEAD_SIZE ** (-0.5) * LOG2E

    @pl.when(step == 0)
    def _():
        @pl.loop(0, length // block)
        def _(part):
            near = pl.ds(pl.multiple_of(part * block, block), block)
            at = pl.ds(pl.multiple_of(swap_chunk(part, per, place_ref[0]) * block, block), block)
            for h, value in enumerate(split_refs(qkv_ref[0, :, near], count)):
                q_t[h, :, at] = grow_rows(value, PAD).astype(jnp.bfloat16)
            for h, value in enumerate(split_refs(qkv_ref[1, :, near], count)):
                k_n[h, at, :] = grow_rows(value, PAD).T.astype(jnp.bfloat16)
            for h, value in enumerate(split_refs(qkv_ref[2, :, near], count)):
                v_t[h, :, at] = grow_rows(value, ROWS).astype(jnp.bfloat16)

    top[...] = jnp.full(top.shape, NEGATIVE, jnp.float32)
    total[...] = jnp.zeros(total.shape, jnp.float32)
    acc[...] = jnp.zeros(acc.shape, jnp.float32)
    query_start = pl.multiple_of(step * block, block)
    queries = pl.ds(query_start, block)

    def first(index, _):
        key_start = pl.multiple_of(index * block, block)
        mask = same_picture(kid_ref, qid_ref, key_start, query_start, block)
        for h in range(count):
            scores = jnp.dot(
                k_n[h, pl.ds(key_start, block), :], q_t[h, :, queries], preferred_element_type=jnp.float32
            )
            scores = jnp.where(mask, scores * factor, NEGATIVE)
            kept[h, pl.ds(key_start, block), :] = scores
            top[h] = jnp.maximum(top[h], jnp.max(scores.reshape(block // 8, 8, block), axis=0))
        return 0

    lax.fori_loop(low_ref[step], high_ref[step], first, 0)
    highest = [jnp.max(top[h], axis=0, keepdims=True) for h in range(count)]

    def second(index, _):
        keys = pl.ds(pl.multiple_of(index * block, block), block)
        for h in range(count):
            probs = jnp.exp2(kept[h, keys, :] - highest[h])
            total[h] += jnp.sum(probs.reshape(block // 8, 8, block), axis=0)
            acc[h] += jnp.dot(v_t[h, :, keys], probs.astype(jnp.bfloat16), preferred_element_type=jnp.float32)
        return 0

    lax.fori_loop(low_ref[step], high_ref[step], second, 0)
    sums = [jnp.sum(total[h], axis=0, keepdims=True) for h in range(count)]
    for h in range(count):
        log_ref[h : h + 1, :] = highest[h] + jnp.log2(sums[h])
    out_ref[0] = jnp.concatenate([acc[h, :HEAD_SIZE] / sums[h] for h in range(count)], axis=0).astype(jnp.bfloat16)


def attend(qkv, low, high, key_ids, query_ids, place, chunk):
    _, width, length = qkv.shape
    count = width // HEAD_SIZE
    block = min(256, chunk)
    per = chunk // block
    whole = lambda *shape: pl.BlockSpec(shape, lambda i, *_: (0,) * len(shape))
    area = length * length * count // 2
    return pl.pallas_call(
        functools.partial(attend_kernel, count=count, block=block, chunk=chunk),
        name="attend",
        grid_spec=pltpu.PrefetchScalarGridSpec(
            num_scalar_prefetch=3,
            grid=(length // block,),
            in_specs=[whole(3, width, length), whole(length, 128), whole(8, length)],
            out_specs=[
                pl.BlockSpec((1, width, block), lambda i, low, high, place: (lax.bitwise_xor(i // per, place[0]), 0, i % per)),
                pl.BlockSpec((max(8, count), block), lambda i, *_: (0, i)),
            ],
            scratch_shapes=[
                pltpu.VMEM((count, PAD, length), jnp.bfloat16),
                pltpu.VMEM((count, length, PAD), jnp.bfloat16),
                pltpu.VMEM((count, ROWS, length), jnp.bfloat16),
                pltpu.VMEM((count, length, block), jnp.float32),
                pltpu.VMEM((count, 8, block), jnp.float32),
                pltpu.VMEM((count, 8, block), jnp.float32),
                pltpu.VMEM((count, ROWS, block), jnp.float32),
            ],
        ),
        out_shape=[
            jax.ShapeDtypeStruct((length // chunk, width, chunk), jnp.bfloat16),
            jax.ShapeDtypeStruct((max(8, count), length), jnp.float32),
        ],
        compiler_params=pltpu.CompilerParams(vmem_limit_bytes=40 << 20),
        cost_estimate=pl.CostEstimate(flops=area * 800, transcendentals=area, bytes_accessed=8 * length * width),
    )(low, high, place, qkv, key_ids, query_ids)


def attend_back_kernel(
    low_ref, high_ref, place_ref, qkv_ref, out_ref, log_ref, kid_ref, qid_ref, *rest, count, block, chunks,
):
    gm_refs, grad_ref = rest[:chunks], rest[chunks]
    q_t, k_t, k_n, v_n, g_t, delta, gq, gk, gv = rest[chunks + 1 :]
    step = pl.program_id(0)
    length = qkv_ref.shape[2]
    chunk = length // chunks
    per = chunk // block
    place = place_ref[0]
    scale = HEAD_SIZE ** (-0.5)
    factor = scale * LOG2E

    @pl.when(step == 0)
    def _():
        gq[...] = jnp.zeros(gq.shape, jnp.float32)

        @pl.loop(0, length // block)
        def _(part):
            near = pl.ds(pl.multiple_of(part * block, block), block)
            at = pl.ds(pl.multiple_of(swap_chunk(part, per, place) * block, block), block)
            for h, value in enumerate(split_refs(qkv_ref[0, :, near], count)):
                q_t[h, :, at] = grow_rows(value, PAD).astype(jnp.bfloat16)
            for h, value in enumerate(split_refs(qkv_ref[1, :, near], count)):
                value = grow_rows(value, PAD)
                k_t[h, :, at] = value[:ROWS].astype(jnp.bfloat16)
                k_n[h, at, :] = value.T.astype(jnp.bfloat16)
            for h, value in enumerate(split_refs(qkv_ref[2, :, near], count)):
                v_n[h, at, :] = grow_rows(value, PAD).T.astype(jnp.bfloat16)

        for piece in range(chunks):
            at = pl.ds(pl.multiple_of(lax.bitwise_xor(piece, place) * chunk, chunk), chunk)
            grads = split_refs(gm_refs[piece][...], count)
            outs = split_refs(out_ref[piece], count)
            for h in range(count):
                g_t[h, :, at] = grow_rows(grads[h], PAD).astype(jnp.bfloat16)
                delta[h, :, at] = jnp.sum(grads[h] * outs[h], axis=0, keepdims=True)

    gk[...] = jnp.zeros(gk.shape, jnp.float32)
    gv[...] = jnp.zeros(gv.shape, jnp.float32)
    key_start = pl.multiple_of(step * block, block)
    keys = pl.ds(key_start, block)

    def one(index, _):
        query_start = pl.multiple_of(index * block, block)
        queries = pl.ds(query_start, block)
        mask = same_picture(kid_ref, qid_ref, key_start, query_start, block)
        for h in range(count):
            scores = jnp.dot(k_n[h, keys, :], q_t[h, :, queries], preferred_element_type=jnp.float32)
            probs = jnp.where(mask, jnp.exp2(scores * factor - log_ref[h : h + 1, queries]), 0.0)
            back = jnp.dot(v_n[h, keys, :], g_t[h, :, queries], preferred_element_type=jnp.float32)
            slope = (probs * (back - delta[h, :, queries])).astype(jnp.bfloat16)
            nt = (((1,), (1,)), ((), ()))
            gv[h] += lax.dot_general(
                g_t[h, :ROWS, queries], probs.astype(jnp.bfloat16), nt, preferred_element_type=jnp.float32
            )
            gk[h] += lax.dot_general(q_t[h, :ROWS, queries], slope, nt, preferred_element_type=jnp.float32)
            gq[h, :, queries] += jnp.dot(k_t[h, :, keys], slope, preferred_element_type=jnp.float32)
        return 0

    lax.fori_loop(low_ref[step], high_ref[step], one, 0)
    near = pl.ds(pl.multiple_of(swap_chunk(step, per, place) * block, block), block)
    grad_ref[1, :, near] = (jnp.concatenate([gk[h, :HEAD_SIZE] for h in range(count)], axis=0) * scale).astype(jnp.bfloat16)
    grad_ref[2, :, near] = jnp.concatenate([gv[h, :HEAD_SIZE] for h in range(count)], axis=0).astype(jnp.bfloat16)

    @pl.when(step == pl.num_programs(0) - 1)
    def _():
        @pl.loop(0, length // block)
        def _(part):
            near = pl.ds(pl.multiple_of(part * block, block), block)
            at = pl.ds(pl.multiple_of(swap_chunk(part, per, place) * block, block), block)
            grad_ref[0, :, near] = (
                jnp.concatenate([gq[h, :HEAD_SIZE, at] for h in range(count)], axis=0) * scale
            ).astype(jnp.bfloat16)


def attend_back(qkv, grad_mixed, mixed, logsum, low, high, key_ids, query_ids, place):
    _, width, length = qkv.shape
    chunk = mixed.shape[2]
    count = width // HEAD_SIZE
    block = min(256, chunk)
    whole = lambda *shape: pl.BlockSpec(shape, lambda i, *_: (0,) * len(shape))
    area = length * length * count // 2
    return pl.pallas_call(
        functools.partial(attend_back_kernel, count=count, block=block, chunks=mixed.shape[0]),
        name="attend_back",
        grid_spec=pltpu.PrefetchScalarGridSpec(
            num_scalar_prefetch=3,
            grid=(length // block,),
            in_specs=[
                whole(3, width, length),
                whole(*mixed.shape),
                whole(max(8, count), length),
                whole(length, 128),
                whole(8, length),
            ]
            + [whole(*piece.shape) for piece in grad_mixed],
            out_specs=whole(3, width, length),
            scratch_shapes=[
                pltpu.VMEM((count, PAD, length), jnp.bfloat16),
                pltpu.VMEM((count, ROWS, length), jnp.bfloat16),
                pltpu.VMEM((count, length, PAD), jnp.bfloat16),
                pltpu.VMEM((count, length, PAD), jnp.bfloat16),
                pltpu.VMEM((count, PAD, length), jnp.bfloat16),
                pltpu.VMEM((count, 1, length), jnp.float32),
                pltpu.VMEM((count, ROWS, length), jnp.float32),
                pltpu.VMEM((count, ROWS, block), jnp.float32),
                pltpu.VMEM((count, ROWS, block), jnp.float32),
            ],
        ),
        out_shape=jax.ShapeDtypeStruct((3, width, length), jnp.bfloat16),
        compiler_params=pltpu.CompilerParams(vmem_limit_bytes=60 << 20),
        cost_estimate=pl.CostEstimate(flops=area * 2000, transcendentals=area, bytes_accessed=16 * length * width),
    )(low, high, place, qkv, mixed, logsum, key_ids, query_ids, *grad_mixed)


def block_ranges(ids, block):
    ids = jnp.where(ids < 0, 1 << 20, ids).reshape(-1, block)
    first, last = ids[:, 0], ids[:, -1]
    low = jnp.sum((last[None, :] < first[:, None]).astype(jnp.int32), axis=1)
    high = jnp.sum((first[None, :] <= last[:, None]).astype(jnp.int32), axis=1)
    return low, high


def norm_parts(value_rows):
    center = value_rows - jnp.mean(value_rows, axis=-1, keepdims=True)
    inverse = lax.rsqrt(jnp.mean(center * center, axis=-1, keepdims=True) + EPS)
    return center * inverse, inverse


def norm_back(grad, normed, inverse, gain):
    scaled = grad * gain
    flat = jnp.mean(scaled, axis=-1, keepdims=True)
    along = jnp.mean(scaled * normed, axis=-1, keepdims=True)
    return inverse * (scaled - flat - normed * along)


def gelu_parts(hidden):
    first, third = math.sqrt(2 / math.pi), 0.044715 * math.sqrt(2 / math.pi)
    square = hidden * hidden
    half = 0.5 + 0.5 * jnp.tanh(hidden * (first + third * square))
    value = hidden * half
    return value, half + 2 * value * (1 - half) * (first + 3 * third * square)


def contract(left, right, left_axis, right_axis):
    return lax.dot_general(left, right, (((left_axis,), (right_axis,)), ((), ())), preferred_element_type=jnp.float32)


def per_device(
    tokens, picture_ids, attn_gain, attn_shift, query_weight, query_bias, key_weight, value_weight, value_bias,
    output_weight, output_bias, mlp_gain, mlp_shift, up_weight, up_bias, down_weight, down_bias, cotangent,
    *, seq_count, row_count,
):
    count, chunk, width = tokens.shape
    length = chunk * seq_count
    part = width // seq_count
    band_width = width // row_count
    hidden_size = up_weight.shape[1]
    slab = -(-hidden_size // (seq_count * 128)) * 128
    place = lax.axis_index("seq")
    place_array = place.reshape(1).astype(jnp.int32)
    block = min(256, chunk)
    f32, bf16 = jnp.float32, jnp.bfloat16
    rest = range(1, seq_count)

    def swap(value, hop):
        return lax.ppermute(value, "seq", [(i, i ^ hop) for i in range(seq_count)])

    def own_columns(weight):
        return lax.dynamic_slice_in_dim(weight, place * part, part, axis=1)

    def relative(stacked):
        return [lax.dynamic_index_in_dim(stacked, place ^ hop, axis=0, keepdims=False) for hop in range(seq_count)]

    whole_rows = [[tokens[row]] for row in range(count)]
    token_rows = [tokens[row] for row in range(count)]
    for row in range(count):
        if row:
            held = lax.optimization_barrier((token_rows[row], *whole_rows[row - 1][1:]))
            token_rows[row], whole_rows[row - 1][1:] = held[0], list(held[1:])
        whole_rows[row] += [swap(token_rows[row], hop) for hop in rest]

    small = [attn_gain, attn_shift, query_bias, value_bias, output_bias, mlp_gain, mlp_shift, down_bias, up_bias]
    sizes = [value.shape[0] for value in small]
    extra_rows = -(-sum(sizes) // (24 * part)) * 8

    def beside(matrix, vectors):
        lead = vectors.shape[:-1]
        vectors = jnp.pad(vectors, [(0, 0)] * len(lead) + [(0, extra_rows * 3 * part - vectors.shape[-1])])
        return jnp.concatenate([matrix, vectors.reshape(*lead, extra_rows, 3 * part)], axis=-2)

    def split(vectors):
        pieces, start = [], 0
        for size in sizes:
            pieces.append(vectors[..., start : start + size])
            start += size
        return pieces

    heads_shard = jnp.concatenate([own_columns(query_weight), own_columns(key_weight), own_columns(value_weight)], axis=1)
    heads_shard = beside(heads_shard, jnp.concatenate(small))
    gathered = lax.all_gather(heads_shard, "rows", axis=0, tiled=False)
    heads_weight = gathered[:, :band_width].reshape(width, 3 * part)
    extra = gathered[:, band_width:].reshape(row_count, extra_rows * 3 * part).astype(f32)
    gain1, shift1, query_off, value_off, output_off, gain2, shift2, down_off, up_off = [
        piece.reshape(-1) for piece in split(extra)
    ]
    up_off = relative(jnp.pad(up_off, (0, slab * seq_count - hidden_size)).reshape(seq_count, slab))
    heads_off = jnp.concatenate(
        [
            lax.dynamic_slice_in_dim(query_off, place * part, part),
            jnp.zeros((part,), f32),
            lax.dynamic_slice_in_dim(value_off, place * part, part),
        ]
    )

    def in_slabs(weight):
        return jnp.pad(weight, ((0, 0), (0, slab * seq_count - hidden_size)))

    def own_slab(weight, hop):
        return lax.dynamic_slice_in_dim(weight, (place ^ hop) * slab, slab, axis=1)

    def near_slabs(weight, hops):
        weight = in_slabs(weight)
        return lax.all_gather(jnp.concatenate([own_slab(weight, hop) for hop in hops], axis=1), "rows", axis=0, tiled=True)

    direct = list(rest)[:2]
    down_turned = down_weight.T
    down_own = near_slabs(down_turned, [0])
    output_whole = lax.all_gather(output_weight, "rows", axis=0, tiled=True)
    halves = [range(seq_count // 2), range(seq_count // 2, seq_count)]
    ups = [near_slabs(up_weight, hops) for hops in halves]
    late = [hop for hop in rest if hop not in direct]
    down_turned, ups[1] = lax.optimization_barrier((down_turned, ups[1]))
    down_late = near_slabs(down_turned, late) if late else None
    up_off = jnp.concatenate(up_off)
    outputs = relative(output_whole.reshape(seq_count, part, width))

    normed_rows, packs, mixes, logs, tables, mixed_own = [], [], [], [], [], []
    for row in range(count):
        ids = picture_ids[row]
        low, high = block_ranges(ids, block)
        ids_table = (jnp.broadcast_to(ids[:, None], (length, 128)), jnp.broadcast_to(ids[None], (8, length)))
        tables.append((low, high, *ids_table))
        normed_pieces = [norm_parts(piece.astype(f32))[0] for piece in whole_rows[row]]
        attn_input = jnp.concatenate([(piece * gain1 + shift1).astype(bf16) for piece in normed_pieces], axis=0)
        normed_rows.append(jnp.concatenate([piece.astype(bf16) for piece in normed_pieces], axis=0))
        pack = (contract(heads_weight, attn_input, 0, 1) + heads_off[:, None]).astype(bf16).reshape(3, part, length)
        mixed, logsum = attend(pack, *tables[row], place_array, chunk)
        packs.append(pack)
        mixes.append(mixed)
        logs.append(logsum)
        mixed_own.append([mixed[0]] + [swap(mixed[hop], hop) for hop in rest])

    held = lax.optimization_barrier((down_own, *mixed_own[-1][1:]))
    down_own, mixed_own[-1][1:] = held[0], list(held[1:])
    downs = [down_own] + [swap(down_own, hop) for hop in direct]
    downs += [down_late[:, i * slab : (i + 1) * slab] for i in range(len(late))]

    mixed_all = jnp.concatenate(
        [jnp.concatenate([mixed_own[row][hop] for row in range(count)], axis=1) for hop in range(seq_count)], axis=0
    )
    output_near = jnp.concatenate(outputs, axis=0)
    tokens_own = tokens.reshape(count * chunk, width).astype(f32)
    resid = tokens_own + (contract(mixed_all, output_near, 0, 0) + output_off)
    normed2, inverse2 = norm_parts(resid)
    mlp_input = (normed2 * gain2 + shift2).astype(bf16)
    parts = []
    for hops, weight in zip(halves, ups):
        offset = up_off[hops[0] * slab : (hops[-1] + 1) * slab]
        parts.append([v.astype(bf16) for v in gelu_parts(contract(mlp_input, weight, 1, 0) + offset)])
    gelu_out = jnp.concatenate([pair[0] for pair in parts], axis=1)
    slope = jnp.concatenate([pair[1] for pair in parts], axis=1)

    def slab_of(value, hop):
        return value[:, hop * slab : (hop + 1) * slab]

    def all_pieces(share):
        stacked = jnp.stack([share] + [swap(share, hop) for hop in rest])
        return relative(stacked)

    def exchange_sum(pieces):
        total = pieces[0].astype(f32)
        for hop in rest:
            total = total + swap(pieces[hop], hop).astype(f32)
        return total

    cot = cotangent.reshape(count * chunk, width)
    grad_down = with_layout_constraint(contract(cot, gelu_out, 0, 0).astype(bf16), Layout(major_to_minor=(0, 1)))
    cot, grad_down = lax.optimization_barrier((cot, grad_down))
    down_raw = lax.psum_scatter(grad_down, "rows", scatter_dimension=0, tiled=True)
    grad_pieces = [(contract(cot, downs[hop], 1, 0) * slab_of(slope, hop).astype(f32)).astype(bf16) for hop in range(seq_count)]
    up_grads = jnp.stack(relative(jnp.stack([jnp.sum(piece.astype(f32), axis=0) for piece in grad_pieces])))
    grad_hidden = jnp.concatenate(grad_pieces, axis=1)
    grad_mlp_input = None
    for hops, weight in zip(halves, ups):
        term = contract(grad_hidden[:, hops[0] * slab : (hops[-1] + 1) * slab], weight, 1, 1)
        grad_mlp_input = term if grad_mlp_input is None else grad_mlp_input + term
    grad_up = contract(mlp_input, grad_hidden, 0, 0).astype(bf16)
    grad_resid = cot.astype(f32) + norm_back(grad_mlp_input, normed2, inverse2, gain2)
    grad_attn = grad_resid.astype(bf16)

    grad_output = contract(mixed_all, grad_attn, 1, 0)
    grad_output = relative(grad_output.astype(bf16).reshape(seq_count, part, width))
    grad_output = jnp.concatenate(grad_output, axis=0)
    mixed_grads = []
    for row in range(count):
        pieces = []
        for hop in range(seq_count):
            piece = contract(outputs[hop], grad_attn[row * chunk : (row + 1) * chunk], 1, 1).astype(bf16)
            pieces.append(swap(piece, hop) if hop else piece)
        mixed_grads.append(pieces)
    held = lax.optimization_barrier((packs[0], down_raw, grad_up, grad_output, *mixed_grads[0]))
    packs[0], down_raw, grad_up, grad_output = held[:4]
    mixed_grads[0] = list(held[4:])
    up_raw = lax.psum_scatter(grad_up, "rows", scatter_dimension=0, tiled=True)
    down_share = exchange_sum([slab_of(down_raw, hop) for hop in range(seq_count)]).astype(bf16)
    down_pieces = all_pieces(down_share)
    normed_grad, sum_grad, grad_in, grad_packs = None, 0.0, [], []
    early_grads = [
        jnp.sum(grad_attn.astype(f32), axis=0),
        jnp.sum(grad_mlp_input * normed2, axis=0),
        jnp.sum(grad_mlp_input, axis=0),
        jnp.sum(cot.astype(f32), axis=0),
        up_grads.reshape(slab * seq_count)[:hidden_size],
    ]
    early_grads = jnp.concatenate([value.reshape(row_count, -1) for value in early_grads], axis=1)
    after = None
    for row in range(count):
        grad_mixed = mixed_grads[row]
        pack = packs[row]
        if after is not None:
            pack, grad_in[-1], early_grads = lax.optimization_barrier((pack, grad_in[-1], early_grads))
        grad_pack = attend_back(pack, grad_mixed, mixes[row], logs[row], *tables[row], place_array)
        if row == count - 1:
            grad_pack, up_raw, grad_output = lax.optimization_barrier((grad_pack, up_raw, grad_output))
            output_share = lax.psum_scatter(grad_output, "rows", scatter_dimension=0, tiled=True)
        grad_pack = grad_pack.reshape(3 * part, length)
        sum_grad = sum_grad + jnp.sum(grad_pack.astype(f32), axis=1)
        partial = []
        for hop in range(seq_count):
            piece = contract(grad_pack[:, hop * chunk : (hop + 1) * chunk], heads_weight, 0, 1)
            partial.append(piece.astype(bf16))
        grad_in.append(partial)
        after = partial
        grad_packs.append(grad_pack)

    held = lax.optimization_barrier((*grad_packs, *grad_in[-1]))
    grad_packs, grad_in[-1] = held[:count], list(held[count:])
    for row in range(count):
        term = with_layout_constraint(contract(normed_rows[row], grad_packs[row], 0, 1), Layout(major_to_minor=(0, 1)))
        normed_grad = term if normed_grad is None else normed_grad + term

    def placed(value):
        return lax.dynamic_update_slice_in_dim(jnp.zeros((width,), f32), value, place * part, axis=0)

    wide_weight = heads_weight.astype(f32)
    heads_grad = gain1[:, None] * normed_grad + shift1[:, None] * sum_grad
    late_grads = [
        jnp.sum(wide_weight * normed_grad, axis=1),
        jnp.sum(wide_weight * sum_grad, axis=1),
        placed(sum_grad[:part]),
        placed(sum_grad[2 * part :]),
    ]
    together = jnp.concatenate([value.reshape(row_count, -1) for value in late_grads] + [early_grads], axis=1).astype(bf16)
    heads_grad = beside(heads_grad.astype(bf16).reshape(row_count, band_width, 3 * part), together)
    held = lax.optimization_barrier((heads_grad, output_share, *[pieces[0] for pieces in grad_in]))
    heads_grad, output_share = held[:2]
    for row in range(count):
        grad_in[row][0] = held[2 + row]
    held = lax.optimization_barrier((gelu_out, output_share, up_raw, heads_grad, *down_pieces))
    gelu_late, output_share, up_raw, heads_grad = held[:4]
    down_pieces = held[4:]
    total = resid
    for hop in range(seq_count):
        total = total + contract(slab_of(gelu_late, hop), downs[hop], 1, 1)
    activations = total + down_off
    up_share = exchange_sum([slab_of(up_raw, hop) for hop in range(seq_count)]).astype(bf16)
    up_pieces = all_pieces(up_share)

    heads_share = lax.psum_scatter(heads_grad, "rows", scatter_dimension=0, tiled=False)
    normed1, inverse1 = norm_parts(tokens_own)
    sums = []
    for row in range(count):
        sums.append(exchange_sum(grad_in[row]))
    grad_attn_input = jnp.concatenate(sums, axis=0)
    token_grad = grad_resid + norm_back(grad_attn_input, normed1, inverse1, gain1)

    def seq_sum(share):
        total = share.astype(f32)
        for hop in rest:
            total = total + swap(share, hop).astype(f32)
        return total

    heads_all = [piece.astype(f32) for piece in all_pieces(heads_share)]
    small_sum = sum(piece[band_width:] for piece in heads_all).reshape(extra_rows * 3 * part)
    vectors = split(small_sum)

    def take(which):
        return jnp.concatenate([piece[:band_width, which * part : (which + 1) * part] for piece in heads_all], axis=1)

    def slabs(pieces):
        return jnp.concatenate([piece.astype(f32) for piece in pieces], axis=1)[:, :hidden_size]

    return (
        activations.reshape(count, chunk, width),
        token_grad.reshape(count, chunk, width),
        vectors[0],
        vectors[1],
        take(0),
        vectors[2],
        take(1),
        take(2),
        vectors[3],
        seq_sum(output_share),
        vectors[4],
        vectors[5],
        vectors[6],
        slabs(up_pieces),
        vectors[8],
        slabs(down_pieces).T,
        vectors[7],
    )


def solution(mesh):
    matrix, vector, batch = P("rows", None), P("rows"), P("rows", "seq", None)
    columns = P(None, "rows")

    def body(*arguments):
        return per_device(*arguments, seq_count=mesh.shape["seq"], row_count=mesh.shape["rows"])

    return jax.shard_map(
        body,
        mesh=mesh,
        in_specs=(
            batch, matrix, vector, vector, matrix, vector, matrix, matrix, vector, matrix, vector, vector, vector, matrix,
            vector, columns, vector, batch,
        ),
        out_specs=(
            batch, batch, vector, vector, matrix, vector, matrix, matrix, vector, matrix, vector, vector, vector, matrix,
            vector, columns, vector,
        ),
        check_vma=False,
    )
```
